32 devices in a mesh: dom: 32 (over z, y, x, core).
Axes of the slice: x: 2, y: 2, z: 4, core: 2. Of those that a mesh axis runs over, the one named last changes fastest.
Arguments:
- right_side: float32 [18, 32768], P(None, 'dom'), may hold values from -20 to 20
- element_matrix: bfloat16 [72, 72, 16384], P(None, None, 'dom'), may hold values from -8 to 8, as said below
- face_map: int32 [4, 16384], P(None, 'dom'), may hold values from 0 to 1535
- share_index: int32 [32, 4, 128], P('dom'), may hold values from 0 to 1023
- share_count: int32 [32, 4], P('dom'), may hold values from 0 to 128, as said below
- face_mass: float32 [32768], P('dom'), may hold values from 0.5 to 2
- absorbing: int32 [32768], P('dom'), may hold values 0 or 1
- impedance: float32 [32768], P('dom'), may hold values from 0.5 to 4
Outputs:
- solution: float32 [18, 32768], P(None, 'dom')
- residual: float32 [18, 32768], P(None, 'dom')
The draws below stay inside these ranges and needn't reach their ends.
Inputs may be any that keep to these rules, and one draw needn't show every extreme that they name: `element_matrix`: each element's 72 x 72 matrix is symmetric positive definite. share_count[d, k] is 0 where device d + o_k lies outside the axis; it equals 128 for some device and offset in every draw.
All inputs are finite; a program needn't handle non-finite values. No bound on the sum of `absorbing` on one device may be relied on, other than what follows from the above.
Results may differ from the reference program's by a relative error of at most 0.0003.
Values sent between devices are 32-bit elements; how exact they have to be, the bound alone decides.
A program may use at most 64 MiB of HBM per device.

```python
import math
import jax
import jax.numpy as jnp
from jax import lax

TRACE = 18
SIDES = 4
DOFS = 72
REACH = 2
OFFSETS = 4
E_DEV = 512
F_DEV = 1024
GH = 128
ITERS = 2
E_TOTAL = 16384
F_TOTAL = 32768
N_DOM = 32


def draw_right_side(key, part):
    devices = F_TOTAL // F_DEV
    first_key, second_key, third_key = jax.random.split(key, 3)
    base_draw = jnp.clip(jax.random.normal(first_key, (TRACE, F_TOTAL), jnp.float32), -4.0, 4.0)
    component = jnp.exp(jax.random.uniform(second_key, (TRACE,), jnp.float32, jnp.log(0.5), jnp.log(5.0)))
    face_scale = jnp.exp(jax.random.uniform(third_key, (F_TOTAL,), jnp.float32, jnp.log(0.3), jnp.log(3.0)))
    device_of = jnp.arange(F_TOTAL, dtype=jnp.int32) // F_DEV
    ramp_scale = jnp.power(3.0, 0.5 * device_of.astype(jnp.float32) / (devices - 1))
    values_out = base_draw * component[:, None] * face_scale[None, :] * ramp_scale[None, :] * 0.25
    return jnp.clip(values_out, -20.0, 20.0).astype(jnp.float32)


def draw_element_matrix(key, part):
    devices = E_TOTAL // E_DEV

    def one_device(part_index):
        device_key = jax.random.fold_in(key, part_index)
        first_key, second_key = jax.random.split(device_key)
        raw_draw = jnp.clip(jax.random.normal(first_key, (DOFS, DOFS, E_DEV), jnp.float32), -5.0, 5.0)
        symmetric = 0.5 * (raw_draw + raw_draw.transpose(1, 0, 2)) * 0.025
        identity = jnp.eye(DOFS, dtype=jnp.float32)[:, :, None]
        off_diag = symmetric * (1.0 - identity)
        rowsum = jnp.sum(jnp.abs(off_diag), axis=1)
        stiffness = jnp.exp(jax.random.uniform(second_key, (E_DEV,), jnp.float32, jnp.log(0.5), jnp.log(2.0)))
        matrix = (off_diag + identity * (rowsum + 0.3)[:, None, :]) * stiffness[None, None, :]
        return matrix.astype(jnp.bfloat16)
    stacked = lax.map(one_device, jnp.arange(devices, dtype=jnp.int32))
    return jnp.moveaxis(stacked, 0, 2).reshape(DOFS, DOFS, E_TOTAL)


def draw_share_count(key, part):
    devices = F_TOTAL // F_DEV
    first_key, second_key, third_key, fourth_key = jax.random.split(key, 4)
    full_draw = jax.random.randint(first_key, (devices, OFFSETS), 0, 4)
    small_draw = jax.random.randint(second_key, (devices, OFFSETS), 0, GH // 4 + 1)
    counts = jnp.where(full_draw == 0, GH, small_draw)
    row_index = lax.broadcasted_iota(jnp.int32, (devices, OFFSETS), 0)
    blocks = lax.broadcasted_iota(jnp.int32, (devices, OFFSETS), 1)
    shift_by = jnp.where(blocks < REACH, blocks - REACH, blocks - REACH + 1)
    inside = (row_index + shift_by >= 0) & (row_index + shift_by < devices)
    pick_row = jax.random.randint(third_key, (), REACH, devices - REACH)
    pick_block = jax.random.randint(fourth_key, (), 0, OFFSETS)
    counts = jnp.where((row_index == pick_row) & (blocks == pick_block), GH, counts)
    return jnp.where(inside, counts, 0).astype(jnp.int32)


def touch_ends(entries, rng, smallest, top_value):
    shape = entries.shape
    index_at = [jax.random.randint(jax.random.fold_in(rng, axis), (), 0, shape[axis]) for axis in range(len(shape))]
    entries = entries.at[tuple(index_at)].set(smallest)
    longest = shape.index(max(shape))
    index_at[longest] = (index_at[longest] + 1) % shape[longest]
    return entries.at[tuple(index_at)].set(top_value)


def level_of(rng, shape, cuts, low, top_value):
    factor_of, own = 1.0, jax.random.fold_in(rng, 6)
    for axis_at, shards_of in cuts:
        heights = jnp.exp(jax.random.uniform(jax.random.fold_in(own, axis_at), (shards_of,), jnp.float32, low / len(cuts), top_value / len(cuts)))
        factor_of = factor_of * jnp.repeat(heights, shape[axis_at] // shards_of).reshape([-1 if axis == axis_at else 1 for axis in range(len(shape))])
    return factor_of


def setup_inputs(seed: int = 0) -> dict:
    streams_of = jax.random.split(jax.random.key(seed), 9)
    right_side = draw_right_side(jax.random.fold_in(streams_of[8], 71), 0)
    element_matrix = draw_element_matrix(jax.random.fold_in(streams_of[8], 71), 0)
    face_map = touch_ends(jax.random.randint(streams_of[2], (SIDES, E_TOTAL), 0, F_DEV + OFFSETS * GH), jax.random.fold_in(streams_of[2], 1), 0, (F_DEV + OFFSETS * GH) - 1).astype(jnp.int32)
    share_index = touch_ends(jax.random.randint(streams_of[3], (N_DOM, OFFSETS, GH), 0, F_DEV), jax.random.fold_in(streams_of[3], 1), 0, F_DEV - 1).astype(jnp.int32)
    share_count = draw_share_count(jax.random.fold_in(streams_of[8], 71), 0)
    face_mass = jnp.clip(jnp.exp(math.log(2.0) - 1.3862944 * jax.random.uniform(streams_of[5], (F_TOTAL,), jnp.float32) ** level_of(streams_of[5], (F_TOTAL,), ((0, 32),), -0.2, 0.2)), 0.5, 2.0)
    absorbing = touch_ends((jax.random.randint(streams_of[6], (F_TOTAL,), 0, 4) < 1).astype(jnp.int32), jax.random.fold_in(streams_of[6], 1), 0, 1)
    impedance = jnp.clip(jnp.exp(math.log(4.0) - 2.0794415 * jax.random.uniform(streams_of[7], (F_TOTAL,), jnp.float32) ** level_of(streams_of[7], (F_TOTAL,), ((0, 32),), -0.2, 0.2)), 0.5, 4.0)
    return {"right_side": right_side, "element_matrix": element_matrix, "face_map": face_map, "share_index": share_index, "share_count": share_count, "face_mass": face_mass, "absorbing": absorbing, "impedance": impedance}


def offset_of(block_index):
    return block_index - REACH if block_index < REACH else block_index - REACH + 1


def slot_map(face_map, share_index, share_count):
    element_count = face_map.shape[1]
    owner = jnp.arange(element_count, dtype=jnp.int32) // E_DEV
    owner = jnp.broadcast_to(owner[None, :], face_map.shape)
    local_face = face_map < F_DEV
    ghost_slot = jnp.maximum(face_map - F_DEV, 0)
    block_index = ghost_slot // GH
    within = ghost_slot % GH
    offsets = jnp.array([offset_of(b) for b in range(OFFSETS)], dtype=jnp.int32)
    sender = owner - offsets[block_index]
    sender_ok = (sender >= 0) & (sender < N_DOM)
    sender_safe = jnp.clip(sender, 0, N_DOM - 1).astype(jnp.int32)
    remote = share_index[sender_safe, block_index, within]
    live_count = share_count[sender_safe, block_index]
    alive_slot = sender_ok & (within < live_count)
    target = jnp.where(local_face, owner * F_DEV + face_map, sender_safe * F_DEV + remote).astype(jnp.int32)
    weight = jnp.where(local_face | alive_slot, 1.0, 0.0).astype(jnp.float32)
    return target, weight


def operate(field_now, element_matrix, target, weight, diagonal):
    picked = field_now[:, target] * weight[None, :, :]
    picked = picked.transpose(1, 0, 2).reshape(DOFS, E_TOTAL)

    def one_part(part_index):
        first_element = part_index * E_DEV
        matrices = lax.dynamic_slice_in_dim(element_matrix, first_element, E_DEV, 2).astype(jnp.float32)
        traces_in = lax.dynamic_slice_in_dim(picked, first_element, E_DEV, 1)
        return jnp.sum(matrices * traces_in[None, :, :], axis=1)

    products = lax.map(one_part, jnp.arange(N_DOM, dtype=jnp.int32))
    product = products.transpose(1, 0, 2).reshape(DOFS, E_TOTAL)
    spread = product.reshape(SIDES, TRACE, E_TOTAL) * weight[:, None, :]
    spread = spread.transpose(1, 0, 2)
    result = jnp.zeros_like(field_now).at[:, target].add(spread)
    return result + diagonal[None, :] * field_now


def reference(right_side, element_matrix, face_map, share_index, share_count, face_mass, absorbing, impedance):
    diagonal = face_mass + absorbing.astype(jnp.float32) * impedance
    target, weight = slot_map(face_map, share_index, share_count)
    solution = jnp.zeros_like(right_side)
    residual = right_side
    direction = right_side
    norm_now = jnp.sum(residual * residual)
    for rounds in range(ITERS):
        image_vec = operate(direction, element_matrix, target, weight, diagonal)
        step_size = norm_now / jnp.sum(direction * image_vec)
        solution = solution + step_size * direction
        residual = residual - step_size * image_vec
        norm_next = jnp.sum(residual * residual)
        direction = residual + (norm_next / norm_now) * direction
        norm_now = norm_next
    return solution, residual
```

```python
import functools
import jax
import jax.numpy as jnp
from jax import lax
from jax.experimental import pallas as pl
from jax.experimental.pallas import tpu as pltpu
from jax.sharding import PartitionSpec as P

LANES = 128
WIDE = 256
MESH = pl.DeviceIdType.MESH
F32 = jnp.float32
BF16 = jnp.bfloat16


def offset_list(block_count):
    half_count = block_count // 2
    return [
        block_index - half_count if block_index < half_count else block_index - half_count + 1
        for block_index in range(block_count)
    ]


def split2(x):
    high = x.astype(BF16)
    low = (x - high.astype(F32)).astype(BF16)
    return jnp.concatenate([high, low], axis=0)


def sum2(x):
    rows = x.shape[0] // 2
    return x[:rows] + x[rows:]


def dot(a, b):
    return lax.dot_general(a, b, (((1,), (0,)), ((), ())), preferred_element_type=F32)


def dot_nt(a, b):
    return lax.dot_general(a, b, (((1,), (1,)), ((), ())), preferred_element_type=F32)


def lane_pick(x, index):
    return jnp.take_along_axis(x, index, axis=1, mode="promise_in_bounds")


def kernel(
    cfg,
    rs_in, em_ref, fm_in, si_in, sc_in, mass_in, absorb_in, imp_in,
    sol_ref, res_ref,
    rs_ref, fm_ref, si_ref, sc_ref, mass_ref, absorb_ref, imp_ref,
    em_buf, pick_map, send_map, same_map, h_send, h_recv,
    own_buf, picked, x_high, x_low, prod, sums,
    in_sem, em_sem, h_send_sem, h_recv_sem, s_send_sem, s_recv_sem,
):
    n, g1, g2, trace, sides, elements, own, blocks, width = cfg
    offsets = offset_list(blocks)
    pad = -(-trace // 8) * 8
    dofs = sides * trace
    own_hi = own // WIDE
    ghost = blocks * width
    ghost_hi = ghost // WIDE
    own_tiles, ghost_tiles = own // LANES, ghost // LANES
    tiles = elements // LANES
    me = lax.axis_index("dom")
    block_of, in_block = me // g1, lax.rem(me, g1)

    barrier = pltpu.get_barrier_semaphore()
    waits = jnp.int32((g1 - 1) + (g2 - 1))
    near = jnp.int32(0)
    for o in offsets:
        there = me + o
        inside = (there >= 0) & (there < n)
        near = near + inside.astype(jnp.int32)

        @pl.when(inside)
        def _():
            pl.semaphore_signal(barrier, inc=1, device_id=(there,), device_id_type=MESH)

    waits = waits + near

    def peer1(d):
        return block_of * g1 + lax.rem(in_block + d, g1)

    def peer2(d):
        return lax.rem(block_of + d, g2) * g1 + in_block

    for d in range(1, g1):
        pl.semaphore_signal(barrier, inc=1, device_id=(peer1(d),), device_id_type=MESH)
    for d in range(1, g2):
        pl.semaphore_signal(barrier, inc=1, device_id=(peer2(d),), device_id_type=MESH)

    in_copies = [
        pltpu.make_async_copy(source, target, in_sem.at[i])
        for i, (source, target) in enumerate(
            (
                (rs_in, rs_ref), (si_in, si_ref), (sc_in, sc_ref), (fm_in, fm_ref),
                (mass_in, mass_ref), (absorb_in, absorb_ref), (imp_in, imp_ref),
            )
        )
    ]
    for copy in in_copies:
        copy.start()
    for t in range(tiles):
        pltpu.make_async_copy(
            em_ref.at[:, pl.ds(t * LANES, LANES)], em_buf.at[t], em_sem
        ).start()

    def piece(ref, i, k):
        return ref.at[i, :, pl.ds(k * width, width)]

    def halo(i, k, step):
        there = me + step
        copy = pltpu.make_async_remote_copy(
            src_ref=piece(h_send, i, k), dst_ref=piece(h_recv, i, k),
            send_sem=h_send_sem, recv_sem=h_recv_sem.at[i],
            device_id=(there,), device_id_type=MESH,
        )
        return copy, (there >= 0) & (there < n)

    far_first = sorted(range(blocks), key=lambda k: -abs(offsets[k]))

    def step_of(i, k):
        return offsets[k] if i % 2 == 0 else -offsets[k]

    def start_all(i):
        for k in far_first:
            copy, to = halo(i, k, step_of(i, k))
            pl.when(to)(copy.start)

    def wait_near(view, sem):
        for count in range(1, blocks + 1):

            @pl.when(near == count)
            def _():
                ref = view(count)
                pltpu.make_async_copy(ref, ref, sem).wait()

    def wait_recv(i):
        wait_near(lambda count: h_recv.at[i, :, pl.ds(0, count * width)], h_recv_sem.at[i])

    for copy in in_copies[:3]:
        copy.wait()

    row_live = lax.broadcasted_iota(jnp.int32, (8, LANES), 0) < trace - (pad - 8)
    own_buf[...] = jnp.zeros_like(own_buf)
    own_buf[0, 0:trace, :] = rs_ref[...]
    slot_iota = lax.broadcasted_iota(jnp.int32, (1, width), 1)
    alive = [slot_iota < sc_ref[0:1, k : k + 1] for k in range(blocks)]
    send_index = [si_ref[0, k : k + 1, :] for k in range(blocks)]

    def pick_tile(source, first_tile, count, index, value):
        low = jnp.broadcast_to(index & (LANES - 1), (pad, LANES))
        high = jnp.broadcast_to(index >> 7, (pad, LANES))
        for h in range(count):
            got = lane_pick(source(h), low)
            value = jnp.where(high == first_tile + h, got, value)
        return value

    def own_tile(rnd):
        return lambda h: own_buf[rnd, :, h * LANES : (h + 1) * LANES]

    def send_values(rnd, k):
        value = pick_tile(
            own_tile(rnd), 0, own_tiles, send_index[k], jnp.zeros((pad, LANES), F32)
        )
        return jnp.where(alive[k], value, 0.0)

    for k in range(blocks):
        h_send[0, :, k * width : (k + 1) * width] = send_values(0, k)
    for k in range(blocks):
        for i in range(4):
            came = me - step_of(i, k)

            @pl.when((came < 0) | (came >= n))
            def _():
                h_recv[i, :, k * width : (k + 1) * width] = jnp.zeros((pad, width), F32)

    pl.semaphore_wait(barrier, waits)
    start_all(0)

    for copy in in_copies[3:]:
        copy.wait()

    def face_index(t, s):
        return fm_ref[s : s + 1, t * LANES : (t + 1) * LANES]

    def pick_own(rnd):
        for t in range(tiles):
            for s in range(sides):
                picked[rnd, t, s] = pick_tile(
                    own_tile(rnd), 0, own_tiles, face_index(t, s), jnp.zeros((pad, LANES), F32)
                )

    pick_own(0)

    lo_iota = lax.broadcasted_iota(jnp.int32, (WIDE, LANES), 0)

    def one_hot(test):
        return jnp.where(test, 1.0, 0.0).astype(BF16)

    for t in range(tiles):
        for s in range(sides):
            lane = (t * sides + s) * LANES
            low = face_index(t, s) & (WIDE - 1)
            pick_map[:, lane : lane + LANES] = one_hot(lo_iota == low)
    for k in range(blocks):
        low = jnp.where(alive[k], send_index[k] & (WIDE - 1), -1)
        send_map[:, k * width : (k + 1) * width] = one_hot(lo_iota == low)
    for a in range(blocks):
        index = jnp.where(alive[a], send_index[a], -2).astype(F32)
        column = jnp.transpose(jnp.broadcast_to(index, (width, width)))
        for k in range(blocks):
            row = jnp.where(alive[k], send_index[k], -1).astype(F32)
            same_map[a * width : (a + 1) * width, k * width : (k + 1) * width] = one_hot(
                column == row
            )
    prod[...] = jnp.zeros_like(prod)
    diag_row = mass_ref[...] + absorb_ref[...].astype(F32) * imp_ref[...]

    pairs = dofs // 2
    body = dofs - 8

    def product(t):
        def row_at(ref, j):
            at = j // trace * pad + j % trace
            return jnp.broadcast_to(ref[t, at : at + 1, :], (8, LANES))

        def run(first, blocks, inputs):
            total = [None] * blocks
            for jj in range(pairs):
                at = jj * 2 * dofs + first
                high, low = (inputs(ref, jj).astype(BF16) for ref in (x_high, x_low))
                for i in range(blocks):
                    matrix = em_buf[t, at + i * 16 : at + i * 16 + 16, :]
                    for x in (high, low):
                        term = matrix.astype(F32) * x.astype(F32)
                        total[i] = term if jj == 0 and x is high else total[i] + term
            return total

        def rows(first, second):
            return lambda ref, jj: jnp.concatenate(
                [row_at(ref, 2 * jj + first), row_at(ref, 2 * jj + second)], axis=0
            )

        even = run(0, body // 16, rows(0, 0))
        odd = run(dofs + 8, body // 16, rows(1, 1))
        mixed = run(body, 1, rows(0, 1))[0]
        return jnp.concatenate(even + [mixed[:8]], axis=0) + jnp.concatenate(
            [mixed[8:]] + odd, axis=0
        )

    def side_values(rnd, t, s):
        value = prod[rnd, t, s * trace : s * trace + pad, :]
        return jnp.concatenate(
            [value[: pad - 8], jnp.where(row_live, value[pad - 8 :], 0.0)], axis=0
        )

    def spread(rnd, t, first_hi, count):
        parts = []
        for s in range(sides):
            value = side_values(rnd, t, s)
            high = jnp.broadcast_to(face_index(t, s) >> 8, (pad, LANES))
            parts.append(
                split2(
                    jnp.concatenate(
                        [jnp.where(high == first_hi + h, value, 0.0) for h in range(count)], axis=0
                    )
                )
            )
        lane = t * sides * LANES
        return dot_nt(
            jnp.concatenate(parts, axis=1), pick_map[:, lane : lane + sides * LANES]
        )

    def elements_of(rnd):
        source = 2 * rnd
        ghost_total = None
        for t in range(tiles):
            for s in range(sides):
                value = pick_tile(
                    lambda h: h_recv[source, :, h * LANES : (h + 1) * LANES],
                    own_tiles, ghost_tiles, face_index(t, s), picked[rnd, t, s],
                )
                picked[rnd, t, s] = value
                high = value.astype(BF16).astype(F32)
                x_high[t, s * pad : (s + 1) * pad, :] = high
                x_low[t, s * pad : (s + 1) * pad, :] = value - high
            prod[rnd, t, 0:dofs, :] = product(t)
        for t in range(tiles):
            part = spread(rnd, t, own_hi, ghost_hi)
            ghost_total = part if ghost_total is None else ghost_total + part
        ghost_total = sum2(ghost_total)
        for h in range(ghost_hi):
            h_send[source + 1, :, h * WIDE : (h + 1) * WIDE] = ghost_total[h * pad : (h + 1) * pad]

    def own_sums(rnd):
        total = None
        for t in range(tiles):
            part = spread(rnd, t, 0, own_hi)
            total = part if total is None else total + part
        total = sum2(total)
        for h in range(own_hi):
            lanes = slice(h * WIDE, (h + 1) * WIDE)
            own_buf[rnd + 1, :, lanes] = (
                total[h * pad : (h + 1) * pad] + own_buf[rnd, :, lanes] * diag_row[:, lanes]
            )

    def add_returned(rnd):
        parts = []
        for k in range(blocks):
            value = h_recv[2 * rnd + 1, :, k * width : (k + 1) * width]
            high = jnp.broadcast_to(send_index[k] >> 8, (pad, LANES))
            parts.append(
                split2(
                    jnp.concatenate(
                        [jnp.where(high == i, value, 0.0) for i in range(own_hi)], axis=0
                    )
                )
            )
        total = sum2(dot_nt(jnp.concatenate(parts, axis=1), send_map[...]))
        for h in range(own_hi):
            lanes = slice(h * WIDE, (h + 1) * WIDE)
            own_buf[rnd + 1, :, lanes] += total[h * pad : (h + 1) * pad]

    def sum_copy(target, slot_here, slot_there, sem):
        return pltpu.make_async_remote_copy(
            src_ref=sums.at[slot_here], dst_ref=sums.at[slot_there],
            send_sem=s_send_sem, recv_sem=s_recv_sem.at[sem],
            device_id=(target,), device_id_type=MESH,
        )

    def sum_wait(first, count, sem):
        ref = sums.at[pl.ds(first, count)]
        pltpu.make_async_copy(ref, ref, sem).wait()

    def lane_sums(x):
        total = jnp.sum(x, axis=0, keepdims=True)
        while total.shape[1] > LANES:
            half = total.shape[1] // 2
            total = total[:, :half] + total[:, half:]
        return total

    def totals(parts):
        total = jnp.sum(jnp.sum(parts, axis=0), axis=1, keepdims=True)
        return total[0:1], total[1:2]

    def begin_sum(x, y):
        sums[in_block] = jnp.concatenate([x, y], axis=0)
        for d in range(1, g1):
            sum_copy(peer1(d), in_block, in_block, 0).start()

    def middle_sum():
        sum_wait(0, g1 - 1, s_recv_sem.at[0])
        sums[g1 + block_of] = jnp.sum(sums[0:g1], axis=0)
        for d in range(1, g2):
            sum_copy(peer2(d), g1 + block_of, g1 + block_of, 1).start()

    def end_sum():
        sum_wait(0, g2 - 1, s_recv_sem.at[1])
        return totals(sums[g1 : g1 + g2])

    def begin_straight(x, y):
        base = g1 + g2
        sums[base] = jnp.concatenate([x, y], axis=0)
        for d in sorted(range(1, n), key=lambda d: abs(2 * d - n)):
            sum_copy(lax.rem(me + d, n), base, base + d, 2).start()

    def end_straight():
        sum_wait(0, n - 1, s_recv_sem.at[2])
        return totals(sums[g1 + g2 : g1 + g2 + n])

    pltpu.make_async_copy(em_buf, em_buf, em_sem).wait()
    wait_recv(0)
    elements_of(0)
    start_all(1)
    b = own_buf[0]
    energy = None
    for t in range(tiles):
        for s in range(sides):
            term = picked[0, t, s] * side_values(0, t, s)
            energy = term if energy is None else energy + term
    begin_sum(lane_sums(b * b), lane_sums(energy) + lane_sums(b * b * diag_row))
    own_sums(0)
    partial_send = [send_values(1, k) for k in range(blocks)]
    for k in range(blocks):
        h_send[2, :, k * width : (k + 1) * width] = partial_send[k]
    wait_recv(1)
    shared = sum2(dot(split2(h_recv[1]), same_map[...]))
    h_send[2] = h_send[2] + shared
    start_all(2)
    middle_sum()
    add_returned(0)
    pick_own(1)

    wait_recv(2)
    elements_of(1)
    start_all(3)
    rr, curve = end_sum()
    step0 = rr / curve
    energy = None
    for t in range(tiles):
        for s in range(sides):
            left = picked[0, t, s] - step0 * picked[1, t, s]
            right = side_values(0, t, s) - step0 * side_values(1, t, s)
            term = left * right
            energy = term if energy is None else energy + term
    r1 = own_buf[0] - step0 * own_buf[1]
    r1_square = r1 * r1
    begin_straight(lane_sums(r1_square), lane_sums(energy) + lane_sums(r1_square * diag_row))
    own_sums(1)
    wait_recv(3)
    add_returned(1)
    new, curve = end_straight()
    beta = new / rr
    step1 = new / (curve - beta * new / step0)
    b, q, w = own_buf[0, 0:trace], own_buf[1, 0:trace], own_buf[2, 0:trace]
    r1 = b - step0 * q
    sol_ref[...] = step0 * b + step1 * (r1 + beta * b)
    res_ref[...] = r1 - step1 * (q - step0 * w + beta * q)
    wait_near(lambda count: h_send.at[:, :, pl.ds(0, count * width)], h_send_sem)
    sum_wait(0, (g1 - 1) + (g2 - 1) + (n - 1), s_send_sem)


def put_out(sol_ref, res_ref, sol_out, res_out, sems):
    copies = [
        pltpu.make_async_copy(sol_ref, sol_out, sems.at[0]),
        pltpu.make_async_copy(res_ref, res_out, sems.at[1]),
    ]
    for copy in copies:
        copy.start()
    for copy in copies:
        copy.wait()


def solution(mesh):
    n = mesh.shape["dom"]
    g1 = next(g for g in range(1, n + 1) if n % g == 0 and g * g >= n)
    g2 = n // g1

    def shards(rs, em, fm, si, sc, mass, absorb, imp):
        trace, own = rs.shape
        sides, elements = fm.shape
        blocks, width = si.shape[1:]
        pad = -(-trace // 8) * 8
        dofs = sides * trace
        tiles = elements // LANES
        ghost = blocks * width
        assert width == LANES and dofs % 16 == 8
        cfg = (n, g1, g2, trace, sides, elements, own, blocks, width)
        dma = pltpu.SemaphoreType.DMA
        vmem = pl.BlockSpec(memory_space=pltpu.VMEM)
        sol, res = pl.pallas_call(
            functools.partial(kernel, cfg),
            out_shape=[pltpu.VMEM(rs.shape, F32)] * 2,
            in_specs=[pl.BlockSpec(memory_space=pltpu.HBM)] * 8,
            out_specs=[vmem] * 2,
            scratch_shapes=[
                pltpu.VMEM(rs.shape, F32),
                pltpu.VMEM(fm.shape, jnp.int32),
                pltpu.VMEM(si.shape, jnp.int32),
                pltpu.VMEM(sc.shape, jnp.int32),
                pltpu.VMEM((1, own), F32),
                pltpu.VMEM((1, own), jnp.int32),
                pltpu.VMEM((1, own), F32),
                pltpu.VMEM((tiles, dofs * dofs, LANES), BF16),
                pltpu.VMEM((WIDE, sides * elements), BF16),
                pltpu.VMEM((WIDE, ghost), BF16),
                pltpu.VMEM((ghost, ghost), BF16),
                pltpu.VMEM((4, pad, ghost), F32),
                pltpu.VMEM((4, pad, ghost), F32),
                pltpu.VMEM((3, pad, own), F32),
                pltpu.VMEM((2, tiles, sides, pad, LANES), F32),
                pltpu.VMEM((tiles, sides * pad, LANES), F32),
                pltpu.VMEM((tiles, sides * pad, LANES), F32),
                pltpu.VMEM((2, tiles, dofs + 8, LANES), F32),
                pltpu.VMEM((g1 + g2 + n, 2, LANES), F32),
                dma((7,)), dma(()), dma(()), dma((4,)), dma(()), dma((3,)),
            ],
            compiler_params=pltpu.CompilerParams(
                collective_id=0, has_side_effects=True, vmem_limit_bytes=62 * 1024 * 1024
            ),
        )(
            rs, em.reshape(dofs * dofs, elements), fm, si, sc,
            mass.reshape(1, own), absorb.reshape(1, own), imp.reshape(1, own),
        )
        return pl.pallas_call(
            put_out,
            out_shape=[jax.ShapeDtypeStruct(rs.shape, F32)] * 2,
            in_specs=[vmem] * 2,
            out_specs=[pl.BlockSpec(memory_space=pltpu.HBM)] * 2,
            scratch_shapes=[dma((2,))],
            compiler_params=pltpu.CompilerParams(vmem_limit_bytes=8 * 1024 * 1024),
        )(sol, res)

    placed = (
        P(None, "dom"),
        P(None, None, "dom"),
        P(None, "dom"),
        P("dom", None, None),
        P("dom", None),
        P("dom"),
        P("dom"),
        P("dom"),
    )
    return jax.shard_map(
        shards,
        mesh=mesh,
        in_specs=placed,
        out_specs=(P(None, "dom"), P(None, "dom")),
        check_vma=False,
    )
```

```python
import functools
import jax
import jax.numpy as jnp
from jax import lax
from jax.experimental import pallas as pl
from jax.experimental.pallas import tpu as pltpu
from jax.sharding import PartitionSpec as P

LANES = 128
WIDE = 256
MESH = pl.DeviceIdType.MESH
F32 = jnp.float32
BF16 = jnp.bfloat16


def offset_list(block_count):
    half_count = block_count // 2
    return [
        block_index - half_count if block_index < half_count else block_index - half_count + 1
        for block_index in range(block_count)
    ]


def split2(x):
    high = x.astype(BF16)
    low = (x - high.astype(F32)).astype(BF16)
    return jnp.concatenate([high, low], axis=0)


def sum2(x):
    rows = x.shape[0] // 2
    return x[:rows] + x[rows:]


def dot(a, b):
    return lax.dot_general(a, b, (((1,), (0,)), ((), ())), preferred_element_type=F32)


def dot_nt(a, b):
    return lax.dot_general(a, b, (((1,), (1,)), ((), ())), preferred_element_type=F32)


def lane_pick(x, index):
    return jnp.take_along_axis(x, index, axis=1, mode="promise_in_bounds")


def kernel(
    cfg,
    rs_in, em_ref, fm_in, si_in, sc_in, mass_in, absorb_in, imp_in,
    sol_ref, res_ref,
    rs_ref, fm_ref, si_ref, sc_ref, mass_ref, absorb_ref, imp_ref,
    em_buf, pick_map, send_map, same_map, pick_same, h_send, h_recv, x_recv,
    own_buf, picked, x_high, x_low, prod, sums,
    in_sem, em_sem, h_send_sem, h_recv_sem, s_send_sem, s_recv_sem, ready,
):
    n, g1, g2, trace, sides, elements, own, blocks, width = cfg
    offsets = offset_list(blocks)
    pad = -(-trace // 8) * 8
    dofs = sides * trace
    own_hi = own // WIDE
    ghost = blocks * width
    ghost_hi = ghost // WIDE
    own_tiles, ghost_tiles = own // LANES, ghost // LANES
    tiles = elements // LANES
    me = lax.axis_index("dom")
    block_of, in_block = me // g1, lax.rem(me, g1)

    barrier = pltpu.get_barrier_semaphore()
    waits = jnp.int32((g1 - 1) + (g2 - 1))
    for o in offsets:
        there = me + o
        inside = (there >= 0) & (there < n)
        waits = waits + inside.astype(jnp.int32)

        @pl.when(inside)
        def _():
            pl.semaphore_signal(barrier, inc=1, device_id=(there,), device_id_type=MESH)

    def peer1(d):
        return block_of * g1 + lax.rem(in_block + d, g1)

    def peer2(d):
        return lax.rem(block_of + d, g2) * g1 + in_block

    for d in range(1, g1):
        pl.semaphore_signal(barrier, inc=1, device_id=(peer1(d),), device_id_type=MESH)
    for d in range(1, g2):
        pl.semaphore_signal(barrier, inc=1, device_id=(peer2(d),), device_id_type=MESH)

    in_copies = [
        pltpu.make_async_copy(source, target, in_sem.at[i])
        for i, (source, target) in enumerate(
            (
                (rs_in, rs_ref), (si_in, si_ref), (sc_in, sc_ref), (fm_in, fm_ref),
                (mass_in, mass_ref), (absorb_in, absorb_ref), (imp_in, imp_ref),
            )
        )
    ]
    for copy in in_copies:
        copy.start()
    for t in range(tiles):
        pltpu.make_async_copy(
            em_ref.at[:, pl.ds(t * LANES, LANES)], em_buf.at[t], em_sem
        ).start()

    def valid(device):
        return (device >= 0) & (device < n)

    def send_piece(source, target, device, i):
        return pltpu.make_async_remote_copy(
            src_ref=source, dst_ref=target,
            send_sem=h_send_sem.at[int(i == 2)], recv_sem=h_recv_sem.at[i],
            device_id=(device,), device_id_type=MESH,
        )

    far_first = sorted(range(blocks), key=lambda k: -abs(offsets[k]))

    def step_of(i, k):
        return offsets[k] if i == 0 else -offsets[k]

    def start_all(i):
        for k in far_first:
            there = me + step_of(i, k)
            copy = send_piece(h_send.at[i, k], h_recv.at[i, k], there, i)
            pl.when(valid(there))(copy.start)

    def relays():
        pairs = [(k, c) for k in range(blocks) for c in range(blocks) if c != k]
        pairs.sort(key=lambda kc: -abs(offsets[kc[1]] - offsets[kc[0]]))
        for k, c in pairs:
            owner = me - offsets[k]
            there = owner + offsets[c]
            copy = send_piece(h_send.at[1, k], x_recv.at[c * blocks + k], there, 2)
            yield copy, valid(owner) & valid(there)

    def owners():
        for k in far_first:
            there = me + offsets[k]
            copy = send_piece(h_send.at[2, k], x_recv.at[k * blocks + k], there, 2)
            yield copy, valid(there)

    def count_of(device, as_count):
        near_count, cross_count = 0, 0
        for k in range(blocks):
            owner = device - offsets[k]
            near_count += as_count(valid(owner))
            for c in range(blocks):
                other = owner + offsets[c]
                cross_count += as_count(valid(owner) & valid(other))
        return near_count, cross_count

    near, cross = count_of(me, lambda test: test.astype(jnp.int32))
    counts = [count_of(device, int) for device in range(n)]

    def wait_count(number, choices, view, sem):
        for count in sorted(set(choices)):

            @pl.when(number == count)
            def _():
                ref = view(count)
                pltpu.make_async_copy(ref, ref, sem).wait()

    near_choices = [pair[0] for pair in counts]
    cross_choices = [pair[1] for pair in counts]

    def wait_recv(i):
        wait_count(
            near, near_choices, lambda count: h_recv.at[i, pl.ds(0, count)], h_recv_sem.at[i]
        )

    for copy in in_copies[:3]:
        copy.wait()

    row_live = lax.broadcasted_iota(jnp.int32, (8, LANES), 0) < trace - (pad - 8)
    own_buf[...] = jnp.zeros_like(own_buf)
    own_buf[0, 0:trace, :] = rs_ref[...]
    slot_iota = lax.broadcasted_iota(jnp.int32, (1, width), 1)
    alive = [slot_iota < sc_ref[0:1, k : k + 1] for k in range(blocks)]
    send_index = [si_ref[0, k : k + 1, :] for k in range(blocks)]

    def pick_tile(source, first_tile, count, index, value):
        low = jnp.broadcast_to(index & (LANES - 1), (pad, LANES))
        high = jnp.broadcast_to(index >> 7, (pad, LANES))
        for h in range(count):
            got = lane_pick(source(h), low)
            value = jnp.where(high == first_tile + h, got, value)
        return value

    def own_tile(rnd):
        return lambda h: own_buf[rnd, :, h * LANES : (h + 1) * LANES]

    def send_values(rnd, k):
        value = pick_tile(
            own_tile(rnd), 0, own_tiles, send_index[k], jnp.zeros((pad, LANES), F32)
        )
        return jnp.where(alive[k], value, 0.0)

    shared_index = [jnp.where(alive[k], send_index[k], -1).astype(F32) for k in range(blocks)]
    for k in range(blocks):
        h_send[0, k] = send_values(0, k)
        for c in range(blocks):
            h_send[0, k, trace + c : trace + c + 1, :] = shared_index[c]

    @pl.when(cross < blocks * blocks)
    def _():
        empty = jnp.zeros((pad, width), F32)
        no_index = jnp.where(
            lax.broadcasted_iota(jnp.int32, (pad, width), 0) < trace, 0.0, -1.0
        )
        for k in range(blocks):
            owner = me - offsets[k]

            @pl.when(~valid(owner))
            def _():
                h_recv[0, k] = no_index

            for i in (1, 3):

                @pl.when(~valid(me - step_of(i, k)))
                def _():
                    h_recv[i, k] = empty

            for c in range(blocks):

                @pl.when(~(valid(owner) & valid(owner + offsets[c])))
                def _():
                    x_recv[k * blocks + c] = empty

    pl.semaphore_wait(barrier, waits)
    start_all(0)
    for d in range(1, g1):
        pl.semaphore_signal(ready, inc=1, device_id=(peer1(d),), device_id_type=MESH)

    for copy in in_copies[3:]:
        copy.wait()

    def face_index(t, s):
        return fm_ref[s : s + 1, t * LANES : (t + 1) * LANES]

    def pick_own(rnd):
        for t in range(tiles):
            for s in range(sides):
                picked[t, s] = pick_tile(
                    own_tile(rnd), 0, own_tiles, face_index(t, s), jnp.zeros((pad, LANES), F32)
                )

    pick_own(0)

    lo_iota = lax.broadcasted_iota(jnp.int32, (WIDE, LANES), 0)

    def one_hot(test):
        return jnp.where(test, 1.0, 0.0).astype(BF16)

    for t in range(tiles):
        for s in range(sides):
            lane = (t * sides + s) * LANES
            low = face_index(t, s) & (WIDE - 1)
            pick_map[:, lane : lane + LANES] = one_hot(lo_iota == low)
    for k in range(blocks):
        low = jnp.where(alive[k], send_index[k] & (WIDE - 1), -1)
        send_map[:, k * width : (k + 1) * width] = one_hot(lo_iota == low)
    prod[...] = jnp.zeros_like(prod)
    diag_row = mass_ref[...] + absorb_ref[...].astype(F32) * imp_ref[...]

    def column_of(row):
        dead_apart = jnp.where(row < 0.0, -2.0, row)
        return jnp.transpose(jnp.broadcast_to(dead_apart, (width, width)))

    def map_shared():
        for k in range(blocks):
            rows = [h_recv[0, k, trace + c : trace + c + 1, :] for c in range(blocks)]
            for c in range(blocks):
                same_map[k, c * width : (c + 1) * width, :] = one_hot(column_of(rows[c]) == rows[k])

    def map_returned():
        for k in range(blocks):
            column = column_of(shared_index[k])
            for t in range(tiles):
                for s in range(sides):
                    lane = (t * sides + s) * LANES
                    pick_same[k * width : (k + 1) * width, lane : lane + LANES] = one_hot(
                        column == face_index(t, s).astype(F32)
                    )

    pairs = dofs // 2
    body = dofs - 8

    def product(t):
        def row_at(ref, j):
            at = j // trace * pad + j % trace
            return jnp.broadcast_to(ref[t, at : at + 1, :], (8, LANES))

        def run(first, blocks, inputs):
            total = [None] * blocks
            for jj in range(pairs):
                at = jj * 2 * dofs + first
                high, low = (inputs(ref, jj).astype(BF16) for ref in (x_high, x_low))
                for i in range(blocks):
                    matrix = em_buf[t, at + i * 16 : at + i * 16 + 16, :]
                    for x in (high, low):
                        term = matrix.astype(F32) * x.astype(F32)
                        total[i] = term if jj == 0 and x is high else total[i] + term
            return total

        def rows(first, second):
            return lambda ref, jj: jnp.concatenate(
                [row_at(ref, 2 * jj + first), row_at(ref, 2 * jj + second)], axis=0
            )

        even = run(0, body // 16, rows(0, 0))
        odd = run(dofs + 8, body // 16, rows(1, 1))
        mixed = run(body, 1, rows(0, 1))[0]
        return jnp.concatenate(even + [mixed[:8]], axis=0) + jnp.concatenate(
            [mixed[8:]] + odd, axis=0
        )

    def side_values(t, s):
        value = prod[t, s * trace : s * trace + pad, :]
        return jnp.concatenate(
            [value[: pad - 8], jnp.where(row_live, value[pad - 8 :], 0.0)], axis=0
        )

    def spread(t, first_hi, count):
        parts = []
        for s in range(sides):
            value = side_values(t, s)
            high = jnp.broadcast_to(face_index(t, s) >> 8, (pad, LANES))
            parts.append(
                split2(
                    jnp.concatenate(
                        [jnp.where(high == first_hi + h, value, 0.0) for h in range(count)], axis=0
                    )
                )
            )
        lane = t * sides * LANES
        return dot_nt(
            jnp.concatenate(parts, axis=1), pick_map[:, lane : lane + sides * LANES]
        )

    def elements_of(rnd):
        ghost_total = None
        for t in range(tiles):
            for s in range(sides):
                value = pick_tile(
                    lambda h: h_recv[2 * rnd, h],
                    own_tiles, ghost_tiles, face_index(t, s), picked[t, s],
                )
                picked[t, s] = value
                high = value.astype(BF16).astype(F32)
                x_high[t, s * pad : (s + 1) * pad, :] = high
                x_low[t, s * pad : (s + 1) * pad, :] = value - high
            prod[t, 0:dofs, :] = product(t)
        for t in range(tiles):
            part = spread(t, own_hi, ghost_hi)
            ghost_total = part if ghost_total is None else ghost_total + part
        ghost_total = sum2(ghost_total)
        per_wide = WIDE // width
        for k in range(blocks):
            h, lane = k // per_wide, k % per_wide * width
            h_send[2 * rnd + 1, k] = ghost_total[h * pad : (h + 1) * pad, lane : lane + width]

    def energy_of():
        energy = None
        for t in range(tiles):
            for s in range(sides):
                term = picked[t, s] * side_values(t, s)
                energy = term if energy is None else energy + term
        return lane_sums(energy)

    def own_sums(rnd):
        total = None
        for t in range(tiles):
            part = spread(t, 0, own_hi)
            total = part if total is None else total + part
        total = sum2(total)
        for h in range(own_hi):
            lanes = slice(h * WIDE, (h + 1) * WIDE)
            own_buf[rnd + 1, :, lanes] = (
                total[h * pad : (h + 1) * pad] + own_buf[rnd, :, lanes] * diag_row[:, lanes]
            )

    def add_returned(rnd):
        parts = []
        for k in range(blocks):
            value = h_recv[2 * rnd + 1, k]
            high = jnp.broadcast_to(send_index[k] >> 8, (pad, LANES))
            parts.append(
                split2(
                    jnp.concatenate(
                        [jnp.where(high == i, value, 0.0) for i in range(own_hi)], axis=0
                    )
                )
            )
        total = sum2(dot_nt(jnp.concatenate(parts, axis=1), send_map[...]))
        for h in range(own_hi):
            lanes = slice(h * WIDE, (h + 1) * WIDE)
            own_buf[rnd + 1, :, lanes] += total[h * pad : (h + 1) * pad]

    def lane_sums(x):
        total = jnp.sum(x, axis=0, keepdims=True)
        while total.shape[1] > LANES:
            half = total.shape[1] // 2
            total = total[:, :half] + total[:, half:]
        return total

    def begin_sum(rows):
        sums[me] = jnp.concatenate(rows, axis=0)
        pl.semaphore_wait(ready, g1 - 1)
        for d in range(n - 1):
            pltpu.make_async_remote_copy(
                src_ref=sums.at[me], dst_ref=sums.at[me],
                send_sem=s_send_sem, recv_sem=s_recv_sem,
                device_id=(d + (d >= me).astype(jnp.int32),), device_id_type=MESH,
            ).start()

    def sum_wait(sem):
        ref = sums.at[pl.ds(0, n - 1)]
        pltpu.make_async_copy(ref, ref, sem).wait()

    def end_sum():
        sum_wait(s_recv_sem)
        total = jnp.sum(jnp.sum(sums[...], axis=0), axis=1, keepdims=True)
        return [total[i : i + 1] for i in range(4)]

    pltpu.make_async_copy(em_buf, em_buf, em_sem).wait()
    wait_recv(0)
    elements_of(0)
    for copy, to in relays():
        pl.when(to)(copy.start)
    start_all(1)
    own_sums(0)
    for k in range(blocks):
        h_send[2, k] = send_values(1, k)
    for copy, to in owners():
        pl.when(to)(copy.start)
    b = own_buf[0]
    b_square = lane_sums(b * b)
    b_energy = energy_of() + lane_sums(b * b * diag_row)
    map_shared()
    map_returned()
    pick_own(1)

    wait_recv(1)
    wait_count(cross, cross_choices, lambda count: x_recv.at[pl.ds(0, count)], h_recv_sem.at[2])
    for k in range(blocks):
        parts = jnp.concatenate(
            [h_send[1, k] if c == k else x_recv[k * blocks + c] for c in range(blocks)], axis=1
        )
        h_recv[2, k] = x_recv[k * blocks + k] + sum2(dot(split2(parts), same_map[k]))
    returned = split2(jnp.concatenate([h_recv[1, k] for k in range(blocks)], axis=1))
    for t in range(tiles):
        lane = t * sides * LANES
        extra = sum2(dot(returned, pick_same[:, lane : lane + sides * LANES]))
        for s in range(sides):
            picked[t, s] += extra[:, s * LANES : (s + 1) * LANES]
    add_returned(0)
    q = own_buf[1]
    q_square = lane_sums(q * q)
    q_diagonal = lane_sums(q * q * diag_row)

    elements_of(1)
    begin_sum([b_square, b_energy, q_square, energy_of() + q_diagonal])
    start_all(3)
    own_sums(1)
    wait_recv(3)
    add_returned(1)
    rr, curve, q_norm, q_energy = end_sum()
    step0 = rr / curve
    new = step0 * step0 * q_norm - rr
    beta = new / rr
    r1_energy = curve - 2.0 * step0 * q_norm + step0 * step0 * q_energy
    step1 = new / (r1_energy - beta * new / step0)
    b, q, w = own_buf[0, 0:trace], own_buf[1, 0:trace], own_buf[2, 0:trace]
    r1 = b - step0 * q
    sol_ref[...] = step0 * b + step1 * (r1 + beta * b)
    res_ref[...] = r1 - step1 * (q - step0 * w + beta * q)
    wait_count(
        near, near_choices, lambda count: h_send.at[pl.ds(0, 3), pl.ds(0, count)], h_send_sem.at[0]
    )
    wait_count(cross, cross_choices, lambda count: x_recv.at[pl.ds(0, count)], h_send_sem.at[1])
    sum_wait(s_send_sem)


def put_out(sol_ref, res_ref, sol_out, res_out, sems):
    copies = [
        pltpu.make_async_copy(sol_ref, sol_out, sems.at[0]),
        pltpu.make_async_copy(res_ref, res_out, sems.at[1]),
    ]
    for copy in copies:
        copy.start()
    for copy in copies:
        copy.wait()


def solution(mesh):
    n = mesh.shape["dom"]
    g1 = next(g for g in range(1, n + 1) if n % g == 0 and g * g >= n)
    g2 = n // g1

    def shards(rs, em, fm, si, sc, mass, absorb, imp):
        trace, own = rs.shape
        sides, elements = fm.shape
        blocks, width = si.shape[1:]
        pad = -(-trace // 8) * 8
        dofs = sides * trace
        tiles = elements // LANES
        ghost = blocks * width
        assert width == LANES and dofs % 16 == 8 and trace + blocks <= pad
        cfg = (n, g1, g2, trace, sides, elements, own, blocks, width)
        dma = pltpu.SemaphoreType.DMA
        vmem = pl.BlockSpec(memory_space=pltpu.VMEM)
        sol, res = pl.pallas_call(
            functools.partial(kernel, cfg),
            out_shape=[pltpu.VMEM(rs.shape, F32)] * 2,
            in_specs=[pl.BlockSpec(memory_space=pltpu.HBM)] * 8,
            out_specs=[vmem] * 2,
            scratch_shapes=[
                pltpu.VMEM(rs.shape, F32),
                pltpu.VMEM(fm.shape, jnp.int32),
                pltpu.VMEM(si.shape, jnp.int32),
                pltpu.VMEM(sc.shape, jnp.int32),
                pltpu.VMEM((1, own), F32),
                pltpu.VMEM((1, own), jnp.int32),
                pltpu.VMEM((1, own), F32),
                pltpu.VMEM((tiles, dofs * dofs, LANES), BF16),
                pltpu.VMEM((WIDE, sides * elements), BF16),
                pltpu.VMEM((WIDE, ghost), BF16),
                pltpu.VMEM((blocks, ghost, width), BF16),
                pltpu.VMEM((ghost, sides * elements), BF16),
                pltpu.VMEM((4, blocks, pad, width), F32),
                pltpu.VMEM((4, blocks, pad, width), F32),
                pltpu.VMEM((blocks * blocks, pad, width), F32),
                pltpu.VMEM((3, pad, own), F32),
                pltpu.VMEM((tiles, sides, pad, LANES), F32),
                pltpu.VMEM((tiles, sides * pad, LANES), F32),
                pltpu.VMEM((tiles, sides * pad, LANES), F32),
                pltpu.VMEM((tiles, dofs + 8, LANES), F32),
                pltpu.VMEM((n, 4, LANES), F32),
                dma((7,)), dma(()), dma((2,)), dma((4,)), dma(()), dma(()),
                pltpu.SemaphoreType.REGULAR,
            ],
            compiler_params=pltpu.CompilerParams(
                collective_id=0, has_side_effects=True, vmem_limit_bytes=62 * 1024 * 1024
            ),
        )(
            rs, em.reshape(dofs * dofs, elements), fm, si, sc,
            mass.reshape(1, own), absorb.reshape(1, own), imp.reshape(1, own),
        )
        return pl.pallas_call(
            put_out,
            out_shape=[jax.ShapeDtypeStruct(rs.shape, F32)] * 2,
            in_specs=[vmem] * 2,
            out_specs=[pl.BlockSpec(memory_space=pltpu.HBM)] * 2,
            scratch_shapes=[dma((2,))],
            compiler_params=pltpu.CompilerParams(vmem_limit_bytes=8 * 1024 * 1024),
        )(sol, res)

    placed = (
        P(None, "dom"),
        P(None, None, "dom"),
        P(None, "dom"),
        P("dom", None, None),
        P("dom", None),
        P("dom"),
        P("dom"),
        P("dom"),
    )
    return jax.shard_map(
        shards,
        mesh=mesh,
        in_specs=placed,
        out_specs=(P(None, "dom"), P(None, "dom")),
        check_vma=False,
    )
```

```python
import functools
import jax
import jax.numpy as jnp
from jax import lax
from jax.experimental import pallas as pl
from jax.experimental.pallas import tpu as pltpu
from jax.sharding import PartitionSpec as P

LANES = 128
WIDE = 256
MESH = pl.DeviceIdType.MESH
F32 = jnp.float32
BF16 = jnp.bfloat16


def offset_list(block_count):
    half_count = block_count // 2
    return [
        block_index - half_count if block_index < half_count else block_index - half_count + 1
        for block_index in range(block_count)
    ]


def split2(x):
    high = x.astype(BF16)
    low = (x - high.astype(F32)).astype(BF16)
    return jnp.concatenate([high, low], axis=0)


def sum2(x):
    rows = x.shape[0] // 2
    return x[:rows] + x[rows:]


def dot(a, b):
    return lax.dot_general(a, b, (((1,), (0,)), ((), ())), preferred_element_type=F32)


def dot_nt(a, b):
    return lax.dot_general(a, b, (((1,), (1,)), ((), ())), preferred_element_type=F32)


def lane_pick(x, index):
    return jnp.take_along_axis(x, index, axis=1, mode="promise_in_bounds")


def kernel(
    cfg,
    rs_in, em_ref, fm_in, si_in, sc_in, mass_in, absorb_in, imp_in,
    sol_ref, res_ref,
    rs_ref, fm_ref, si_ref, sc_ref, mass_ref, absorb_ref, imp_ref,
    em_buf, pick_map, send_map, same_map, pick_same, h_send, h_recv, x_recv,
    own_buf, picked, x_high, x_low, prod, sums,
    in_sem, em_sem, h_send_sem, h_recv_sem, s_send_sem, s_recv_sem, ready,
):
    n, trace, sides, elements, own, blocks, width = cfg
    offsets = offset_list(blocks)
    pad = -(-trace // 8) * 8
    dofs = sides * trace
    own_hi = own // WIDE
    ghost = blocks * width
    ghost_hi = ghost // WIDE
    own_tiles, ghost_tiles = own // LANES, ghost // LANES
    tiles = elements // LANES
    me = lax.axis_index("dom")

    barrier = pltpu.get_barrier_semaphore()
    def valid(device):
        return (device >= 0) & (device < n)

    def signal(device, semaphore):
        @pl.when(valid(device))
        def _():
            pl.semaphore_signal(semaphore, inc=1, device_id=(device,), device_id_type=MESH)

    def count_valid(*devices):
        return sum(valid(device).astype(jnp.int32) for device in devices)

    for o in offsets:
        signal(me + o, barrier)

    reaches = []
    reach = 2 * max(offsets)
    while reach < n - 1:
        reaches.append(reach)
        reach *= 2

    def spread_word(i):
        for device in (me - reaches[i], me + reaches[i]):
            signal(device, ready.at[i])

    def hear_word(i):
        count = count_valid(me - reaches[i], me + reaches[i])
        pl.semaphore_wait(ready.at[i], count)

    def pass_word(i):
        if i < len(reaches):
            hear_word(i)
        if i + 1 < len(reaches):
            spread_word(i + 1)

    in_copies = [
        pltpu.make_async_copy(source, target, in_sem.at[i])
        for i, (source, target) in enumerate(
            (
                (rs_in, rs_ref), (si_in, si_ref), (sc_in, sc_ref), (fm_in, fm_ref),
                (mass_in, mass_ref), (absorb_in, absorb_ref), (imp_in, imp_ref),
            )
        )
    ]
    for copy in in_copies:
        copy.start()
    for t in range(tiles):
        pltpu.make_async_copy(
            em_ref.at[:, pl.ds(t * LANES, LANES)], em_buf.at[t], em_sem
        ).start()

    def live(ref, i):
        return ref if i == 0 else ref.at[pl.ds(0, trace)]

    def send_piece(source, target, device, i):
        return pltpu.make_async_remote_copy(
            src_ref=live(source, i), dst_ref=live(target, i),
            send_sem=h_send_sem.at[(0, 1, 2, 1)[i]], recv_sem=h_recv_sem.at[i],
            device_id=(device,), device_id_type=MESH,
        )

    far_first = sorted(range(blocks), key=lambda k: -abs(offsets[k]))

    def step_of(i, k):
        return offsets[k] if i == 0 else -offsets[k]

    def start_all(i):
        for k in far_first:
            there = me + step_of(i, k)
            copy = send_piece(h_send.at[i, k], h_recv.at[i, k], there, i)
            pl.when(valid(there))(copy.start)

    def relays():
        pairs = [(k, c) for k in range(blocks) for c in range(blocks) if c != k]
        pairs.sort(key=lambda kc: -abs(offsets[kc[1]] - offsets[kc[0]]))
        for k, c in pairs:
            owner = me - offsets[k]
            there = owner + offsets[c]
            copy = send_piece(h_send.at[1, k], x_recv.at[c * blocks + k], there, 2)
            yield copy, valid(owner) & valid(there)

    def owners():
        for k in far_first:
            there = me + offsets[k]
            copy = send_piece(h_send.at[2, k], x_recv.at[k * blocks + k], there, 2)
            yield copy, valid(there)

    def count_of(device, as_count):
        near_count, cross_count = 0, 0
        for k in range(blocks):
            owner = device - offsets[k]
            near_count += as_count(valid(owner))
            for c in range(blocks):
                other = owner + offsets[c]
                cross_count += as_count(valid(owner) & valid(other))
        return near_count, cross_count

    near, cross = count_of(me, lambda test: test.astype(jnp.int32))
    counts = [count_of(device, int) for device in range(n)]

    def wait_count(number, choices, view, sem):
        for count in sorted(set(choices)):

            @pl.when(number == count)
            def _():
                ref = view(count)
                pltpu.make_async_copy(ref, ref, sem).wait()

    near_choices = [pair[0] for pair in counts]
    cross_choices = [pair[1] for pair in counts]

    def wait_recv(i):
        rows = pad if i == 0 else trace
        wait_count(
            near,
            near_choices,
            lambda count: h_recv.at[i, pl.ds(0, count), pl.ds(0, rows)],
            h_recv_sem.at[i],
        )

    def cross_view(count):
        return x_recv.at[pl.ds(0, count), pl.ds(0, trace)]

    for copy in in_copies[:3]:
        copy.wait()

    row_live = lax.broadcasted_iota(jnp.int32, (8, LANES), 0) < trace - (pad - 8)
    own_buf[...] = jnp.zeros_like(own_buf)
    own_buf[0, 0:trace, :] = rs_ref[...]
    slot_iota = lax.broadcasted_iota(jnp.int32, (1, width), 1)
    alive = [slot_iota < sc_ref[0:1, k : k + 1] for k in range(blocks)]
    send_index = [si_ref[0, k : k + 1, :] for k in range(blocks)]

    def pick_tile(source, first_tile, count, index, value):
        low = jnp.broadcast_to(index & (LANES - 1), (pad, LANES))
        high = jnp.broadcast_to(index >> 7, (pad, LANES))
        for h in range(count):
            got = lane_pick(source(h), low)
            value = jnp.where(high == first_tile + h, got, value)
        return value

    def own_tile(rnd):
        return lambda h: own_buf[rnd, :, h * LANES : (h + 1) * LANES]

    def send_values(rnd, k):
        value = pick_tile(
            own_tile(rnd), 0, own_tiles, send_index[k], jnp.zeros((pad, LANES), F32)
        )
        return jnp.where(alive[k], value, 0.0)

    shared_index = [jnp.where(alive[k], send_index[k], -1).astype(F32) for k in range(blocks)]
    for k in range(blocks):
        h_send[0, k] = send_values(0, k)
        for c in range(blocks):
            h_send[0, k, trace + c : trace + c + 1, :] = shared_index[c]

    dead_rows = jnp.zeros((pad - trace, width), F32)
    for k in range(blocks):
        for i in (1, 3):
            h_recv[i, k, trace:pad, :] = dead_rows
        for c in range(blocks):
            x_recv[k * blocks + c, trace:pad, :] = dead_rows

    @pl.when(cross < blocks * blocks)
    def _():
        empty = jnp.zeros((pad, width), F32)
        no_index = jnp.where(
            lax.broadcasted_iota(jnp.int32, (pad, width), 0) < trace, 0.0, -1.0
        )
        for k in range(blocks):
            owner = me - offsets[k]

            @pl.when(~valid(owner))
            def _():
                h_recv[0, k] = no_index

            for i in (1, 3):

                @pl.when(~valid(me - step_of(i, k)))
                def _():
                    h_recv[i, k] = empty

            for c in range(blocks):

                @pl.when(~(valid(owner) & valid(owner + offsets[c])))
                def _():
                    x_recv[k * blocks + c] = empty

    pl.semaphore_wait(barrier, count_valid(*(me + o for o in offsets)))
    start_all(0)

    for copy in in_copies[3:]:
        copy.wait()

    def face_index(t, s):
        return fm_ref[s : s + 1, t * LANES : (t + 1) * LANES]

    def pick_own(rnd):
        for t in range(tiles):
            for s in range(sides):
                picked[t, s] = pick_tile(
                    own_tile(rnd), 0, own_tiles, face_index(t, s), jnp.zeros((pad, LANES), F32)
                )

    pick_own(0)

    lo_iota = lax.broadcasted_iota(jnp.int32, (WIDE, LANES), 0)

    def one_hot(test):
        return jnp.where(test, 1.0, 0.0).astype(BF16)

    for t in range(tiles):
        for s in range(sides):
            lane = (t * sides + s) * LANES
            low = face_index(t, s) & (WIDE - 1)
            pick_map[:, lane : lane + LANES] = one_hot(lo_iota == low)
    for k in range(blocks):
        low = jnp.where(alive[k], send_index[k] & (WIDE - 1), -1)
        send_map[:, k * width : (k + 1) * width] = one_hot(lo_iota == low)
    prod[...] = jnp.zeros_like(prod)
    diag_row = mass_ref[...] + absorb_ref[...].astype(F32) * imp_ref[...]

    def column_of(row):
        dead_apart = jnp.where(row < 0.0, -2.0, row)
        return jnp.transpose(jnp.broadcast_to(dead_apart, (width, width)))

    def map_shared():
        for k in range(blocks):
            rows = [h_recv[0, k, trace + c : trace + c + 1, :] for c in range(blocks)]
            for c in range(blocks):
                same_map[k, c * width : (c + 1) * width, :] = one_hot(column_of(rows[c]) == rows[k])

    def map_returned():
        for k in range(blocks):
            column = column_of(shared_index[k])
            for t in range(tiles):
                for s in range(sides):
                    lane = (t * sides + s) * LANES
                    pick_same[k * width : (k + 1) * width, lane : lane + LANES] = one_hot(
                        column == face_index(t, s).astype(F32)
                    )

    pairs = dofs // 2
    body = dofs - 8

    def product(t):
        def row_at(ref, j):
            at = j // trace * pad + j % trace
            return jnp.broadcast_to(ref[t, at : at + 1, :], (8, LANES))

        def run(first, blocks, inputs):
            total = [None] * blocks
            for jj in range(pairs):
                at = jj * 2 * dofs + first
                high, low = (inputs(ref, jj).astype(BF16) for ref in (x_high, x_low))
                for i in range(blocks):
                    matrix = em_buf[t, at + i * 16 : at + i * 16 + 16, :]
                    for x in (high, low):
                        term = matrix.astype(F32) * x.astype(F32)
                        total[i] = term if jj == 0 and x is high else total[i] + term
            return total

        def rows(first, second):
            return lambda ref, jj: jnp.concatenate(
                [row_at(ref, 2 * jj + first), row_at(ref, 2 * jj + second)], axis=0
            )

        even = run(0, body // 16, rows(0, 0))
        odd = run(dofs + 8, body // 16, rows(1, 1))
        mixed = run(body, 1, rows(0, 1))[0]
        return jnp.concatenate(even + [mixed[:8]], axis=0) + jnp.concatenate(
            [mixed[8:]] + odd, axis=0
        )

    def side_values(t, s):
        value = prod[t, s * trace : s * trace + pad, :]
        return jnp.concatenate(
            [value[: pad - 8], jnp.where(row_live, value[pad - 8 :], 0.0)], axis=0
        )

    def spread(t, first_hi, count):
        parts = []
        for s in range(sides):
            value = side_values(t, s)
            high = jnp.broadcast_to(face_index(t, s) >> 8, (pad, LANES))
            parts.append(
                split2(
                    jnp.concatenate(
                        [jnp.where(high == first_hi + h, value, 0.0) for h in range(count)], axis=0
                    )
                )
            )
        lane = t * sides * LANES
        return dot_nt(
            jnp.concatenate(parts, axis=1), pick_map[:, lane : lane + sides * LANES]
        )

    def elements_of(rnd, before_tile, after_products):
        ghost_total = None
        for t in range(tiles):
            before_tile(t)
            for s in range(sides):
                value = pick_tile(
                    lambda h: h_recv[2 * rnd, h],
                    own_tiles, ghost_tiles, face_index(t, s), picked[t, s],
                )
                picked[t, s] = value
                high = value.astype(BF16).astype(F32)
                x_high[t, s * pad : (s + 1) * pad, :] = high
                x_low[t, s * pad : (s + 1) * pad, :] = value - high
            prod[t, 0:dofs, :] = product(t)
        result = after_products()
        for t in range(tiles):
            part = spread(t, own_hi, ghost_hi)
            ghost_total = part if ghost_total is None else ghost_total + part
        ghost_total = sum2(ghost_total)
        per_wide = WIDE // width
        for k in range(blocks):
            h, lane = k // per_wide, k % per_wide * width
            h_send[2 * rnd + 1, k] = ghost_total[h * pad : (h + 1) * pad, lane : lane + width]
        return result

    def energy_of():
        energy = None
        for t in range(tiles):
            for s in range(sides):
                term = picked[t, s] * side_values(t, s)
                energy = term if energy is None else energy + term
        return lane_sums(energy)

    def own_sums(rnd):
        total = None
        for t in range(tiles):
            part = spread(t, 0, own_hi)
            total = part if total is None else total + part
        total = sum2(total)
        for h in range(own_hi):
            lanes = slice(h * WIDE, (h + 1) * WIDE)
            own_buf[rnd + 1, :, lanes] = (
                total[h * pad : (h + 1) * pad] + own_buf[rnd, :, lanes] * diag_row[:, lanes]
            )

    def add_returned(rnd):
        parts = []
        for k in range(blocks):
            value = h_recv[2 * rnd + 1, k]
            high = jnp.broadcast_to(send_index[k] >> 8, (pad, LANES))
            parts.append(
                split2(
                    jnp.concatenate(
                        [jnp.where(high == i, value, 0.0) for i in range(own_hi)], axis=0
                    )
                )
            )
        total = sum2(dot_nt(jnp.concatenate(parts, axis=1), send_map[...]))
        for h in range(own_hi):
            lanes = slice(h * WIDE, (h + 1) * WIDE)
            own_buf[rnd + 1, :, lanes] += total[h * pad : (h + 1) * pad]

    def lane_sums(x):
        total = jnp.sum(x, axis=0, keepdims=True)
        while total.shape[1] > LANES:
            half = total.shape[1] // 2
            total = total[:, :half] + total[:, half:]
        return total

    def begin_sum(rows):
        sums[me] = jnp.concatenate(rows, axis=0)
        for d in range(n - 1):
            pltpu.make_async_remote_copy(
                src_ref=sums.at[me], dst_ref=sums.at[me],
                send_sem=s_send_sem, recv_sem=s_recv_sem,
                device_id=(d + (d >= me).astype(jnp.int32),), device_id_type=MESH,
            ).start()

    def sum_wait(sem):
        ref = sums.at[pl.ds(0, n - 1)]
        pltpu.make_async_copy(ref, ref, sem).wait()

    def end_sum():
        sum_wait(s_recv_sem)
        total = jnp.sum(jnp.sum(sums[...], axis=0), axis=1, keepdims=True)
        return [total[i : i + 1] for i in range(4)]

    pltpu.make_async_copy(em_buf, em_buf, em_sem).wait()
    wait_recv(0)
    if reaches:
        spread_word(0)
    elements_of(0, lambda t: None, lambda: None)
    for copy, to in relays():
        pl.when(to)(copy.start)
    start_all(1)
    own_sums(0)
    for k in range(blocks):
        h_send[2, k] = send_values(1, k)
    for copy, to in owners():
        pl.when(to)(copy.start)
    pass_word(0)
    b = own_buf[0]
    b_square = lane_sums(b * b)
    b_energy = energy_of() + lane_sums(b * b * diag_row)
    map_shared()
    map_returned()
    pick_own(1)
    pass_word(1)

    wait_recv(1)
    wait_count(cross, cross_choices, cross_view, h_recv_sem.at[2])
    for k in range(blocks):
        parts = jnp.concatenate(
            [h_send[1, k] if c == k else x_recv[k * blocks + c] for c in range(blocks)], axis=1
        )
        h_recv[2, k] = x_recv[k * blocks + k] + sum2(dot(split2(parts), same_map[k]))
    returned = split2(jnp.concatenate([h_recv[1, k] for k in range(blocks)], axis=1))

    def take_returned(t):
        lane = t * sides * LANES
        extra = sum2(dot(returned, pick_same[:, lane : lane + sides * LANES]))
        for s in range(sides):
            picked[t, s] += extra[:, s * LANES : (s + 1) * LANES]

    def finish_q():
        add_returned(0)
        q = own_buf[1]
        return lane_sums(q * q), lane_sums(q * q * diag_row)

    q_square, q_diagonal = elements_of(1, take_returned, finish_q)
    start_all(3)
    for i in range(2, len(reaches)):
        pass_word(i)
    begin_sum([b_square, b_energy, q_square, energy_of() + q_diagonal])
    own_sums(1)
    wait_recv(3)
    add_returned(1)
    rr, curve, q_norm, q_energy = end_sum()
    step0 = rr / curve
    new = step0 * step0 * q_norm - rr
    beta = new / rr
    r1_energy = curve - 2.0 * step0 * q_norm + step0 * step0 * q_energy
    step1 = new / (r1_energy - beta * new / step0)
    b, q, w = own_buf[0, 0:trace], own_buf[1, 0:trace], own_buf[2, 0:trace]
    r1 = b - step0 * q
    sol_ref[...] = step0 * b + step1 * (r1 + beta * b)
    res_ref[...] = r1 - step1 * (q - step0 * w + beta * q)
    wait_count(near, near_choices, lambda count: h_send.at[0, pl.ds(0, count)], h_send_sem.at[0])
    wait_count(
        near,
        near_choices,
        lambda count: h_send.at[pl.ds(1, 2), pl.ds(0, count), pl.ds(0, trace)],
        h_send_sem.at[1],
    )
    wait_count(cross, cross_choices, cross_view, h_send_sem.at[2])
    sum_wait(s_send_sem)


def put_out(sol_ref, res_ref, sol_out, res_out, sems):
    copies = [
        pltpu.make_async_copy(sol_ref, sol_out, sems.at[0]),
        pltpu.make_async_copy(res_ref, res_out, sems.at[1]),
    ]
    for copy in copies:
        copy.start()
    for copy in copies:
        copy.wait()


def solution(mesh):
    n = mesh.shape["dom"]

    def shards(rs, em, fm, si, sc, mass, absorb, imp):
        trace, own = rs.shape
        sides, elements = fm.shape
        blocks, width = si.shape[1:]
        pad = -(-trace // 8) * 8
        dofs = sides * trace
        tiles = elements // LANES
        ghost = blocks * width
        words = max(1, n.bit_length())
        assert width == LANES and dofs % 16 == 8 and trace + blocks <= pad
        cfg = (n, trace, sides, elements, own, blocks, width)
        dma = pltpu.SemaphoreType.DMA
        vmem = pl.BlockSpec(memory_space=pltpu.VMEM)
        sol, res = pl.pallas_call(
            functools.partial(kernel, cfg),
            out_shape=[pltpu.VMEM(rs.shape, F32)] * 2,
            in_specs=[pl.BlockSpec(memory_space=pltpu.HBM)] * 8,
            out_specs=[vmem] * 2,
            scratch_shapes=[
                pltpu.VMEM(rs.shape, F32),
                pltpu.VMEM(fm.shape, jnp.int32),
                pltpu.VMEM(si.shape, jnp.int32),
                pltpu.VMEM(sc.shape, jnp.int32),
                pltpu.VMEM((1, own), F32),
                pltpu.VMEM((1, own), jnp.int32),
                pltpu.VMEM((1, own), F32),
                pltpu.VMEM((tiles, dofs * dofs, LANES), BF16),
                pltpu.VMEM((WIDE, sides * elements), BF16),
                pltpu.VMEM((WIDE, ghost), BF16),
                pltpu.VMEM((blocks, ghost, width), BF16),
                pltpu.VMEM((ghost, sides * elements), BF16),
                pltpu.VMEM((4, blocks, pad, width), F32),
                pltpu.VMEM((4, blocks, pad, width), F32),
                pltpu.VMEM((blocks * blocks, pad, width), F32),
                pltpu.VMEM((3, pad, own), F32),
                pltpu.VMEM((tiles, sides, pad, LANES), F32),
                pltpu.VMEM((tiles, sides * pad, LANES), F32),
                pltpu.VMEM((tiles, sides * pad, LANES), F32),
                pltpu.VMEM((tiles, dofs + 8, LANES), F32),
                pltpu.VMEM((n, 4, LANES), F32),
                dma((7,)), dma(()), dma((3,)), dma((4,)), dma(()), dma(()),
                pltpu.SemaphoreType.REGULAR((words,)),
            ],
            compiler_params=pltpu.CompilerParams(
                collective_id=0, has_side_effects=True, vmem_limit_bytes=62 * 1024 * 1024
            ),
        )(
            rs, em.reshape(dofs * dofs, elements), fm, si, sc,
            mass.reshape(1, own), absorb.reshape(1, own), imp.reshape(1, own),
        )
        return pl.pallas_call(
            put_out,
            out_shape=[jax.ShapeDtypeStruct(rs.shape, F32)] * 2,
            in_specs=[vmem] * 2,
            out_specs=[pl.BlockSpec(memory_space=pltpu.HBM)] * 2,
            scratch_shapes=[dma((2,))],
            compiler_params=pltpu.CompilerParams(vmem_limit_bytes=8 * 1024 * 1024),
        )(sol, res)

    placed = (
        P(None, "dom"),
        P(None, None, "dom"),
        P(None, "dom"),
        P("dom", None, None),
        P("dom", None),
        P("dom"),
        P("dom"),
        P("dom"),
    )
    return jax.shard_map(
        shards,
        mesh=mesh,
        in_specs=placed,
        out_specs=(P(None, "dom"), P(None, "dom")),
        check_vma=False,
    )
```

```python
import functools
import jax
import jax.numpy as jnp
from jax import lax
from jax.experimental import pallas as pl
from jax.experimental.pallas import tpu as pltpu
from jax.sharding import PartitionSpec as P

LANES = 128
WIDE = 256
MESH = pl.DeviceIdType.MESH
F32 = jnp.float32
BF16 = jnp.bfloat16


def offset_list(block_count):
    half_count = block_count // 2
    return [
        block_index - half_count if block_index < half_count else block_index - half_count + 1
        for block_index in range(block_count)
    ]


def split2(x):
    high = x.astype(BF16)
    low = (x - high.astype(F32)).astype(BF16)
    return jnp.concatenate([high, low], axis=0)


def sum2(x):
    rows = x.shape[0] // 2
    return x[:rows] + x[rows:]


def dot(a, b):
    return lax.dot_general(a, b, (((1,), (0,)), ((), ())), preferred_element_type=F32)


def dot_nt(a, b):
    return lax.dot_general(a, b, (((1,), (1,)), ((), ())), preferred_element_type=F32)


def lane_pick(x, index):
    return jnp.take_along_axis(x, index, axis=1, mode="promise_in_bounds")


def kernel(
    cfg,
    rs_in, em_ref, fm_in, si_in, sc_in, mass_in, absorb_in, imp_in,
    sol_ref, res_ref,
    rs_ref, fm_ref, si_ref, sc_ref, mass_ref, absorb_ref, imp_ref,
    em_buf, pick_map, send_map, same_map, pick_same, h_send, h_recv, x_recv,
    own_buf, picked, x_high, x_low, prod, sums,
    in_sem, em_sem, h_send_sem, h_recv_sem, s_send_sem, s_recv_sem, ready,
):
    n, trace, sides, elements, own, blocks, width = cfg
    offsets = offset_list(blocks)
    pad = -(-trace // 8) * 8
    dofs = sides * trace
    own_hi = own // WIDE
    ghost = blocks * width
    ghost_hi = ghost // WIDE
    own_tiles, ghost_tiles = own // LANES, ghost // LANES
    tiles = elements // LANES
    me = lax.axis_index("dom")

    barrier = pltpu.get_barrier_semaphore()
    def valid(device):
        return (device >= 0) & (device < n)

    def signal(device, semaphore):
        @pl.when(valid(device))
        def _():
            pl.semaphore_signal(semaphore, inc=1, device_id=(device,), device_id_type=MESH)

    def count_valid(*devices):
        return sum(valid(device).astype(jnp.int32) for device in devices)

    for o in offsets:
        signal(me + o, barrier)

    reaches = []
    reach = 2 * max(offsets)
    while reach < n - 1:
        reaches.append(reach)
        reach *= 2

    def spread_word(i):
        for device in (me - reaches[i], me + reaches[i]):
            signal(device, ready.at[i])

    def hear_word(i):
        count = count_valid(me - reaches[i], me + reaches[i])
        pl.semaphore_wait(ready.at[i], count)

    def pass_word(i):
        if i < len(reaches):
            hear_word(i)
        if i + 1 < len(reaches):
            spread_word(i + 1)

    in_copies = [
        pltpu.make_async_copy(source, target, in_sem.at[i])
        for i, (source, target) in enumerate(
            (
                (rs_in, rs_ref), (si_in, si_ref), (sc_in, sc_ref), (fm_in, fm_ref),
                (mass_in, mass_ref), (absorb_in, absorb_ref), (imp_in, imp_ref),
            )
        )
    ]
    for copy in in_copies:
        copy.start()
    for t in range(tiles):
        pltpu.make_async_copy(
            em_ref.at[:, pl.ds(t * LANES, LANES)], em_buf.at[t], em_sem
        ).start()

    def live(ref, i):
        return ref if i == 0 else ref.at[pl.ds(0, trace)]

    def send_piece(source, target, device, i):
        return pltpu.make_async_remote_copy(
            src_ref=live(source, i), dst_ref=live(target, i),
            send_sem=h_send_sem.at[(0, 1, 2, 1)[i]], recv_sem=h_recv_sem.at[i],
            device_id=(device,), device_id_type=MESH,
        )

    far_first = sorted(range(blocks), key=lambda k: -abs(offsets[k]))

    def step_of(i, k):
        return offsets[k] if i == 0 else -offsets[k]

    def start_all(i):
        for k in far_first:
            there = me + step_of(i, k)
            copy = send_piece(h_send.at[i, k], h_recv.at[i, k], there, i)
            pl.when(valid(there))(copy.start)

    def relays():
        pairs = [(k, c) for k in range(blocks) for c in range(blocks) if c != k]
        pairs.sort(key=lambda kc: -abs(offsets[kc[1]] - offsets[kc[0]]))
        for k, c in pairs:
            owner = me - offsets[k]
            there = owner + offsets[c]
            copy = send_piece(h_send.at[1, k], x_recv.at[c * blocks + k], there, 2)
            yield copy, valid(owner) & valid(there)

    def owners():
        for k in far_first:
            there = me + offsets[k]
            copy = send_piece(h_send.at[2, k], x_recv.at[k * blocks + k], there, 2)
            yield copy, valid(there)

    def count_of(device, as_count):
        near_count, cross_count = 0, 0
        for k in range(blocks):
            owner = device - offsets[k]
            near_count += as_count(valid(owner))
            for c in range(blocks):
                other = owner + offsets[c]
                cross_count += as_count(valid(owner) & valid(other))
        return near_count, cross_count

    near, cross = count_of(me, lambda test: test.astype(jnp.int32))
    counts = [count_of(device, int) for device in range(n)]

    def wait_count(number, choices, view, sem):
        for count in sorted(set(choices)):

            @pl.when(number == count)
            def _():
                ref = view(count)
                pltpu.make_async_copy(ref, ref, sem).wait()

    near_choices = [pair[0] for pair in counts]
    cross_choices = [pair[1] for pair in counts]

    def wait_recv(i):
        rows = pad if i == 0 else trace
        wait_count(
            near,
            near_choices,
            lambda count: h_recv.at[i, pl.ds(0, count), pl.ds(0, rows)],
            h_recv_sem.at[i],
        )

    def cross_view(count):
        return x_recv.at[pl.ds(0, count), pl.ds(0, trace)]

    for copy in in_copies[:3]:
        copy.wait()

    row_live = lax.broadcasted_iota(jnp.int32, (8, LANES), 0) < trace - (pad - 8)
    own_buf[...] = jnp.zeros_like(own_buf)
    own_buf[0, 0:trace, :] = rs_ref[...]
    slot_iota = lax.broadcasted_iota(jnp.int32, (1, width), 1)
    alive = [slot_iota < sc_ref[0:1, k : k + 1] for k in range(blocks)]
    send_index = [si_ref[0, k : k + 1, :] for k in range(blocks)]

    def pick_tile(source, first_tile, count, index, value):
        low = jnp.broadcast_to(index & (LANES - 1), (pad, LANES))
        high = jnp.broadcast_to(index >> 7, (pad, LANES))
        for h in range(count):
            got = lane_pick(source(h), low)
            value = jnp.where(high == first_tile + h, got, value)
        return value

    def own_tile(rnd):
        return lambda h: own_buf[rnd, :, h * LANES : (h + 1) * LANES]

    def send_values(rnd, k):
        value = pick_tile(
            own_tile(rnd), 0, own_tiles, send_index[k], jnp.zeros((pad, LANES), F32)
        )
        return jnp.where(alive[k], value, 0.0)

    shared_index = [jnp.where(alive[k], send_index[k], -1).astype(F32) for k in range(blocks)]
    for k in range(blocks):
        h_send[0, k] = send_values(0, k)
        for c in range(blocks):
            h_send[0, k, trace + c : trace + c + 1, :] = shared_index[c]

    dead_rows = jnp.zeros((pad - trace, width), F32)
    for k in range(blocks):
        for i in (1, 3):
            h_recv[i, k, trace:pad, :] = dead_rows
        for c in range(blocks):
            x_recv[k * blocks + c, trace:pad, :] = dead_rows

    @pl.when(cross < blocks * blocks)
    def _():
        empty = jnp.zeros((pad, width), F32)
        no_index = jnp.where(
            lax.broadcasted_iota(jnp.int32, (pad, width), 0) < trace, 0.0, -1.0
        )
        for k in range(blocks):
            owner = me - offsets[k]

            @pl.when(~valid(owner))
            def _():
                h_recv[0, k] = no_index

            for i in (1, 3):

                @pl.when(~valid(me - step_of(i, k)))
                def _():
                    h_recv[i, k] = empty

            for c in range(blocks):

                @pl.when(~(valid(owner) & valid(owner + offsets[c])))
                def _():
                    x_recv[k * blocks + c] = empty

    pl.semaphore_wait(barrier, count_valid(*(me + o for o in offsets)))
    start_all(0)

    for copy in in_copies[3:]:
        copy.wait()

    def face_index(t, s):
        return fm_ref[s : s + 1, t * LANES : (t + 1) * LANES]

    def pick_own(rnd):
        for t in range(tiles):
            for s in range(sides):
                picked[t, s] = pick_tile(
                    own_tile(rnd), 0, own_tiles, face_index(t, s), jnp.zeros((pad, LANES), F32)
                )

    pick_own(0)

    lo_iota = lax.broadcasted_iota(jnp.int32, (WIDE, LANES), 0)

    def one_hot(test):
        return jnp.where(test, 1.0, 0.0).astype(BF16)

    for t in range(tiles):
        for s in range(sides):
            lane = (t * sides + s) * LANES
            low = face_index(t, s) & (WIDE - 1)
            pick_map[:, lane : lane + LANES] = one_hot(lo_iota == low)
    for k in range(blocks):
        low = jnp.where(alive[k], send_index[k] & (WIDE - 1), -1)
        send_map[:, k * width : (k + 1) * width] = one_hot(lo_iota == low)
    prod[...] = jnp.zeros_like(prod)
    diag_row = mass_ref[...] + absorb_ref[...].astype(F32) * imp_ref[...]

    def column_of(row):
        dead_apart = jnp.where(row < 0.0, -2.0, row)
        return jnp.transpose(jnp.broadcast_to(dead_apart, (width, width)))

    def map_shared():
        for k in range(blocks):
            rows = [h_recv[0, k, trace + c : trace + c + 1, :] for c in range(blocks)]
            for c in range(blocks):
                same_map[k, c * width : (c + 1) * width, :] = one_hot(column_of(rows[c]) == rows[k])

    def map_returned():
        for k in range(blocks):
            column = column_of(shared_index[k])
            for t in range(tiles):
                for s in range(sides):
                    lane = (t * sides + s) * LANES
                    pick_same[k * width : (k + 1) * width, lane : lane + LANES] = one_hot(
                        column == face_index(t, s).astype(F32)
                    )

    pairs = dofs // 2
    body = dofs - 8

    def product(t):
        def row_at(ref, j):
            at = j // trace * pad + j % trace
            return jnp.broadcast_to(ref[t, at : at + 1, :], (8, LANES))

        def run(first, blocks, inputs):
            total = [None] * blocks
            for jj in range(pairs):
                at = jj * 2 * dofs + first
                high, low = (inputs(ref, jj).astype(BF16) for ref in (x_high, x_low))
                for i in range(blocks):
                    matrix = em_buf[t, at + i * 16 : at + i * 16 + 16, :]
                    for x in (high, low):
                        term = matrix.astype(F32) * x.astype(F32)
                        total[i] = term if jj == 0 and x is high else total[i] + term
            return total

        def rows(first, second):
            return lambda ref, jj: jnp.concatenate(
                [row_at(ref, 2 * jj + first), row_at(ref, 2 * jj + second)], axis=0
            )

        even = run(0, body // 16, rows(0, 0))
        odd = run(dofs + 8, body // 16, rows(1, 1))
        mixed = run(body, 1, rows(0, 1))[0]
        return jnp.concatenate(even + [mixed[:8]], axis=0) + jnp.concatenate(
            [mixed[8:]] + odd, axis=0
        )

    def side_values(t, s):
        value = prod[t, s * trace : s * trace + pad, :]
        return jnp.concatenate(
            [value[: pad - 8], jnp.where(row_live, value[pad - 8 :], 0.0)], axis=0
        )

    def spread(t, first_hi, count):
        parts = []
        for s in range(sides):
            value = side_values(t, s)
            high = jnp.broadcast_to(face_index(t, s) >> 8, (pad, LANES))
            parts.append(
                split2(
                    jnp.concatenate(
                        [jnp.where(high == first_hi + h, value, 0.0) for h in range(count)], axis=0
                    )
                )
            )
        lane = t * sides * LANES
        return dot_nt(
            jnp.concatenate(parts, axis=1), pick_map[:, lane : lane + sides * LANES]
        )

    def elements_of(rnd):
        ghost_total = None
        for t in range(tiles):
            for s in range(sides):
                value = pick_tile(
                    lambda h: h_recv[2 * rnd, h],
                    own_tiles, ghost_tiles, face_index(t, s), picked[t, s],
                )
                picked[t, s] = value
                high = value.astype(BF16).astype(F32)
                x_high[t, s * pad : (s + 1) * pad, :] = high
                x_low[t, s * pad : (s + 1) * pad, :] = value - high
            prod[t, 0:dofs, :] = product(t)
        for t in range(tiles):
            part = spread(t, own_hi, ghost_hi)
            ghost_total = part if ghost_total is None else ghost_total + part
        ghost_total = sum2(ghost_total)
        per_wide = WIDE // width
        for k in range(blocks):
            h, lane = k // per_wide, k % per_wide * width
            h_send[2 * rnd + 1, k] = ghost_total[h * pad : (h + 1) * pad, lane : lane + width]

    def energy_of():
        energy = None
        for t in range(tiles):
            for s in range(sides):
                term = picked[t, s] * side_values(t, s)
                energy = term if energy is None else energy + term
        return lane_sums(energy)

    def own_sums(rnd):
        total = None
        for t in range(tiles):
            part = spread(t, 0, own_hi)
            total = part if total is None else total + part
        total = sum2(total)
        for h in range(own_hi):
            lanes = slice(h * WIDE, (h + 1) * WIDE)
            own_buf[rnd + 1, :, lanes] = (
                total[h * pad : (h + 1) * pad] + own_buf[rnd, :, lanes] * diag_row[:, lanes]
            )

    def add_returned(rnd):
        parts = []
        for k in range(blocks):
            value = h_recv[2 * rnd + 1, k]
            high = jnp.broadcast_to(send_index[k] >> 8, (pad, LANES))
            parts.append(
                split2(
                    jnp.concatenate(
                        [jnp.where(high == i, value, 0.0) for i in range(own_hi)], axis=0
                    )
                )
            )
        total = sum2(dot_nt(jnp.concatenate(parts, axis=1), send_map[...]))
        for h in range(own_hi):
            lanes = slice(h * WIDE, (h + 1) * WIDE)
            own_buf[rnd + 1, :, lanes] += total[h * pad : (h + 1) * pad]

    def lane_sums(x):
        total = jnp.sum(x, axis=0, keepdims=True)
        while total.shape[1] > LANES:
            half = total.shape[1] // 2
            total = total[:, :half] + total[:, half:]
        return total

    lane_of = lax.broadcasted_iota(jnp.int32, (1, LANES), 1)
    quarter = LANES // 4
    lane_parts = (
        lane_of < quarter,
        (lane_of >= quarter) & (lane_of < 2 * quarter),
        lane_of >= 2 * quarter,
    )

    def fold(x, lanes):
        x = jnp.broadcast_to(x, (8, LANES))
        size = LANES // 2
        while size >= lanes:
            x = x + pltpu.roll(x, size, 1)
            size //= 2
        return x[0:1]

    def one_row(x, y, z):
        rest = jnp.where(lane_parts[1], fold(y, quarter), fold(z, 2 * quarter))
        return jnp.where(lane_parts[0], fold(x, quarter), rest)

    def begin_sum(rows):
        sums[me] = jnp.concatenate(rows, axis=0)
        for d in range(n - 1):
            pltpu.make_async_remote_copy(
                src_ref=sums.at[me], dst_ref=sums.at[me],
                send_sem=s_send_sem, recv_sem=s_recv_sem,
                device_id=(d + (d >= me).astype(jnp.int32),), device_id_type=MESH,
            ).start()

    def sum_wait(sem):
        ref = sums.at[pl.ds(0, n - 1)]
        pltpu.make_async_copy(ref, ref, sem).wait()

    def end_sum():
        sum_wait(s_recv_sem)
        total = jnp.sum(sums[...], axis=0)
        first = total[0:1]
        rows = [jnp.where(part, first, 0.0) for part in lane_parts] + [total[1:2]]
        total = jnp.sum(jnp.concatenate(rows, axis=0), axis=1, keepdims=True)
        return [total[i : i + 1] for i in range(4)]

    pltpu.make_async_copy(em_buf, em_buf, em_sem).wait()
    wait_recv(0)
    if reaches:
        spread_word(0)
    elements_of(0)
    start_all(1)
    for copy, to in relays():
        pl.when(to)(copy.start)
    own_sums(0)
    for k in range(blocks):
        h_send[2, k] = send_values(1, k)
    for copy, to in owners():
        pl.when(to)(copy.start)
    pass_word(0)
    b = own_buf[0]
    b_square = lane_sums(b * b)
    b_energy = energy_of() + lane_sums(b * b * diag_row)
    map_shared()
    map_returned()
    pick_own(1)
    pass_word(1)

    wait_recv(1)
    returned = split2(jnp.concatenate([h_recv[1, k] for k in range(blocks)], axis=1))
    for t in range(tiles):
        lane = t * sides * LANES
        extra = sum2(dot(returned, pick_same[:, lane : lane + sides * LANES]))
        for s in range(sides):
            picked[t, s] += extra[:, s * LANES : (s + 1) * LANES]
    add_returned(0)
    q = own_buf[1]
    q_square = lane_sums(q * q)
    q_diagonal = lane_sums(q * q * diag_row)
    early_row = one_row(b_square, b_energy, q_square)
    wait_count(cross, cross_choices, cross_view, h_recv_sem.at[2])
    for k in range(blocks):
        parts = jnp.concatenate(
            [h_send[1, k] if c == k else x_recv[k * blocks + c] for c in range(blocks)], axis=1
        )
        h_recv[2, k] = x_recv[k * blocks + k] + sum2(dot(split2(parts), same_map[k]))

    elements_of(1)
    start_all(3)
    for i in range(2, len(reaches)):
        pass_word(i)
    begin_sum([early_row, energy_of() + q_diagonal])
    own_sums(1)
    wait_recv(3)
    add_returned(1)
    rr, curve, q_norm, q_energy = end_sum()
    step0 = rr / curve
    new = step0 * step0 * q_norm - rr
    beta = new * (1.0 / rr)
    r1_energy = curve - 2.0 * step0 * q_norm + step0 * step0 * q_energy
    step1 = new / (r1_energy - beta * beta * curve)
    b, q, w = own_buf[0, 0:trace], own_buf[1, 0:trace], own_buf[2, 0:trace]
    r1 = b - step0 * q
    sol_ref[...] = step0 * b + step1 * (r1 + beta * b)
    res_ref[...] = r1 - step1 * (q - step0 * w + beta * q)
    wait_count(near, near_choices, lambda count: h_send.at[0, pl.ds(0, count)], h_send_sem.at[0])
    wait_count(
        near,
        near_choices,
        lambda count: h_send.at[pl.ds(1, 2), pl.ds(0, count), pl.ds(0, trace)],
        h_send_sem.at[1],
    )
    wait_count(cross, cross_choices, cross_view, h_send_sem.at[2])
    sum_wait(s_send_sem)


def put_out(sol_ref, res_ref, sol_out, res_out, sems):
    copies = [
        pltpu.make_async_copy(sol_ref, sol_out, sems.at[0]),
        pltpu.make_async_copy(res_ref, res_out, sems.at[1]),
    ]
    for copy in copies:
        copy.start()
    for copy in copies:
        copy.wait()


def solution(mesh):
    n = mesh.shape["dom"]

    def shards(rs, em, fm, si, sc, mass, absorb, imp):
        trace, own = rs.shape
        sides, elements = fm.shape
        blocks, width = si.shape[1:]
        pad = -(-trace // 8) * 8
        dofs = sides * trace
        tiles = elements // LANES
        ghost = blocks * width
        words = sum(2 * (blocks // 2) << i < n - 1 for i in range(n)) or 1
        assert width == LANES and dofs % 16 == 8 and trace + blocks <= pad
        cfg = (n, trace, sides, elements, own, blocks, width)
        dma = pltpu.SemaphoreType.DMA
        vmem = pl.BlockSpec(memory_space=pltpu.VMEM)
        sol, res = pl.pallas_call(
            functools.partial(kernel, cfg),
            out_shape=[pltpu.VMEM(rs.shape, F32)] * 2,
            in_specs=[pl.BlockSpec(memory_space=pltpu.HBM)] * 8,
            out_specs=[vmem] * 2,
            scratch_shapes=[
                pltpu.VMEM(rs.shape, F32),
                pltpu.VMEM(fm.shape, jnp.int32),
                pltpu.VMEM(si.shape, jnp.int32),
                pltpu.VMEM(sc.shape, jnp.int32),
                pltpu.VMEM((1, own), F32),
                pltpu.VMEM((1, own), jnp.int32),
                pltpu.VMEM((1, own), F32),
                pltpu.VMEM((tiles, dofs * dofs, LANES), BF16),
                pltpu.VMEM((WIDE, sides * elements), BF16),
                pltpu.VMEM((WIDE, ghost), BF16),
                pltpu.VMEM((blocks, ghost, width), BF16),
                pltpu.VMEM((ghost, sides * elements), BF16),
                pltpu.VMEM((4, blocks, pad, width), F32),
                pltpu.VMEM((4, blocks, pad, width), F32),
                pltpu.VMEM((blocks * blocks, pad, width), F32),
                pltpu.VMEM((3, pad, own), F32),
                pltpu.VMEM((tiles, sides, pad, LANES), F32),
                pltpu.VMEM((tiles, sides * pad, LANES), F32),
                pltpu.VMEM((tiles, sides * pad, LANES), F32),
                pltpu.VMEM((tiles, dofs + 8, LANES), F32),
                pltpu.VMEM((n, 2, LANES), F32),
                dma((7,)), dma(()), dma((3,)), dma((4,)), dma(()), dma(()),
                pltpu.SemaphoreType.REGULAR((words,)),
            ],
            compiler_params=pltpu.CompilerParams(
                collective_id=0, has_side_effects=True, vmem_limit_bytes=62 * 1024 * 1024
            ),
        )(
            rs, em.reshape(dofs * dofs, elements), fm, si, sc,
            mass.reshape(1, own), absorb.reshape(1, own), imp.reshape(1, own),
        )
        return pl.pallas_call(
            put_out,
            out_shape=[jax.ShapeDtypeStruct(rs.shape, F32)] * 2,
            in_specs=[vmem] * 2,
            out_specs=[pl.BlockSpec(memory_space=pltpu.HBM)] * 2,
            scratch_shapes=[dma((2,))],
            compiler_params=pltpu.CompilerParams(vmem_limit_bytes=8 * 1024 * 1024),
        )(sol, res)

    placed = (
        P(None, "dom"),
        P(None, None, "dom"),
        P(None, "dom"),
        P("dom", None, None),
        P("dom", None),
        P("dom"),
        P("dom"),
        P("dom"),
    )
    return jax.shard_map(
        shards,
        mesh=mesh,
        in_specs=placed,
        out_specs=(P(None, "dom"), P(None, "dom")),
        check_vma=False,
    )
```

```python
import functools
import jax
import jax.numpy as jnp
from jax import lax
from jax.experimental import pallas as pl
from jax.experimental.pallas import tpu as pltpu
from jax.sharding import PartitionSpec as P

LANES = 128
WIDE = 256
MESH = pl.DeviceIdType.MESH
F32 = jnp.float32
BF16 = jnp.bfloat16


def offset_list(block_count):
    half_count = block_count // 2
    return [
        block_index - half_count if block_index < half_count else block_index - half_count + 1
        for block_index in range(block_count)
    ]


def split2(x):
    high = x.astype(BF16)
    low = (x - high.astype(F32)).astype(BF16)
    return jnp.concatenate([high, low], axis=0)


def sum2(x):
    rows = x.shape[0] // 2
    return x[:rows] + x[rows:]


def dot(a, b):
    return lax.dot_general(a, b, (((1,), (0,)), ((), ())), preferred_element_type=F32)


def dot_nt(a, b):
    return lax.dot_general(a, b, (((1,), (1,)), ((), ())), preferred_element_type=F32)


def lane_pick(x, index):
    return jnp.take_along_axis(x, index, axis=1, mode="promise_in_bounds")


def kernel(
    cfg,
    rs_in, em_ref, fm_in, si_in, sc_in, mass_in, absorb_in, imp_in,
    sol_ref, res_ref,
    rs_ref, fm_ref, si_ref, sc_ref, mass_ref, absorb_ref, imp_ref,
    em_buf, pick_map, send_map, same_map, pick_same, h_send, h_recv, x_recv,
    own_buf, picked, x_high, x_low, prod, sums,
    in_sem, em_sem, h_send_sem, h_recv_sem, s_send_sem, s_recv_sem, ready,
):
    n, trace, sides, elements, own, blocks, width = cfg
    offsets = offset_list(blocks)
    pad = -(-trace // 8) * 8
    dofs = sides * trace
    own_hi = own // WIDE
    ghost = blocks * width
    ghost_hi = ghost // WIDE
    own_tiles, ghost_tiles = own // LANES, ghost // LANES
    tiles = elements // LANES
    me = lax.axis_index("dom")

    barrier = pltpu.get_barrier_semaphore()
    def valid(device):
        return (device >= 0) & (device < n)

    def signal(device, semaphore):
        @pl.when(valid(device))
        def _():
            pl.semaphore_signal(semaphore, inc=1, device_id=(device,), device_id_type=MESH)

    def count_valid(*devices):
        return sum(valid(device).astype(jnp.int32) for device in devices)

    for o in offsets:
        signal(me + o, barrier)

    reaches = []
    reach = 2 * max(offsets)
    while reach < n - 1:
        reaches.append(reach)
        reach *= 2

    def spread_word(i):
        for device in (me - reaches[i], me + reaches[i]):
            signal(device, ready.at[i])

    def hear_word(i):
        count = count_valid(me - reaches[i], me + reaches[i])
        pl.semaphore_wait(ready.at[i], count)

    def pass_word(i):
        if i < len(reaches):
            hear_word(i)
        if i + 1 < len(reaches):
            spread_word(i + 1)

    in_copies = [
        pltpu.make_async_copy(source, target, in_sem.at[i])
        for i, (source, target) in enumerate(
            (
                (rs_in, rs_ref), (si_in, si_ref), (sc_in, sc_ref), (fm_in, fm_ref),
                (mass_in, mass_ref), (absorb_in, absorb_ref), (imp_in, imp_ref),
            )
        )
    ]
    for copy in in_copies:
        copy.start()
    for t in range(tiles):
        pltpu.make_async_copy(
            em_ref.at[:, pl.ds(t * LANES, LANES)], em_buf.at[t], em_sem
        ).start()

    def live(ref, i):
        return ref if i == 0 else ref.at[pl.ds(0, trace)]

    def send_piece(source, target, device, i):
        return pltpu.make_async_remote_copy(
            src_ref=live(source, i), dst_ref=live(target, i),
            send_sem=h_send_sem.at[(0, 1, 2, 1)[i]], recv_sem=h_recv_sem.at[i],
            device_id=(device,), device_id_type=MESH,
        )

    far_first = sorted(range(blocks), key=lambda k: -abs(offsets[k]))

    def step_of(i, k):
        return offsets[k] if i == 0 else -offsets[k]

    def start_all(i):
        for k in far_first:
            there = me + step_of(i, k)
            copy = send_piece(h_send.at[i, k], h_recv.at[i, k], there, i)
            pl.when(valid(there))(copy.start)

    def relays():
        pairs = [(k, c) for k in range(blocks) for c in range(blocks) if c != k]
        pairs.sort(key=lambda kc: -abs(offsets[kc[1]] - offsets[kc[0]]))
        for k, c in pairs:
            owner = me - offsets[k]
            there = owner + offsets[c]
            copy = send_piece(h_send.at[1, k], x_recv.at[c * blocks + k], there, 2)
            yield copy, valid(owner) & valid(there)

    def owners():
        for k in far_first:
            there = me + offsets[k]
            copy = send_piece(h_send.at[2, k], x_recv.at[k * blocks + k], there, 2)
            yield copy, valid(there)

    def count_of(device, as_count):
        near_count, cross_count = 0, 0
        for k in range(blocks):
            owner = device - offsets[k]
            near_count += as_count(valid(owner))
            for c in range(blocks):
                other = owner + offsets[c]
                cross_count += as_count(valid(owner) & valid(other))
        return near_count, cross_count

    near, cross = count_of(me, lambda test: test.astype(jnp.int32))
    counts = [count_of(device, int) for device in range(n)]

    def wait_count(number, choices, view, sem):
        for count in sorted(set(choices)):

            @pl.when(number == count)
            def _():
                ref = view(count)
                pltpu.make_async_copy(ref, ref, sem).wait()

    near_choices = [pair[0] for pair in counts]
    cross_choices = [pair[1] for pair in counts]

    def wait_recv(i):
        rows = pad if i == 0 else trace
        wait_count(
            near,
            near_choices,
            lambda count: h_recv.at[i, pl.ds(0, count), pl.ds(0, rows)],
            h_recv_sem.at[i],
        )

    def cross_view(count):
        return x_recv.at[pl.ds(0, count), pl.ds(0, trace)]

    for copy in in_copies[:3]:
        copy.wait()

    row_live = lax.broadcasted_iota(jnp.int32, (8, LANES), 0) < trace - (pad - 8)
    own_buf[...] = jnp.zeros_like(own_buf)
    own_buf[0, 0:trace, :] = rs_ref[...]
    slot_iota = lax.broadcasted_iota(jnp.int32, (1, width), 1)
    alive = [slot_iota < sc_ref[0:1, k : k + 1] for k in range(blocks)]
    send_index = [si_ref[0, k : k + 1, :] for k in range(blocks)]

    def pick_tile(source, first_tile, count, index, value):
        low = jnp.broadcast_to(index & (LANES - 1), (pad, LANES))
        high = jnp.broadcast_to(index >> 7, (pad, LANES))
        for h in range(count):
            got = lane_pick(source(h), low)
            value = jnp.where(high == first_tile + h, got, value)
        return value

    def own_tile(rnd):
        return lambda h: own_buf[rnd, :, h * LANES : (h + 1) * LANES]

    def send_values(rnd, k):
        value = pick_tile(
            own_tile(rnd), 0, own_tiles, send_index[k], jnp.zeros((pad, LANES), F32)
        )
        return jnp.where(alive[k], value, 0.0)

    shared_index = [jnp.where(alive[k], send_index[k], -1).astype(F32) for k in range(blocks)]
    for k in range(blocks):
        h_send[0, k] = send_values(0, k)
        for c in range(blocks):
            h_send[0, k, trace + c : trace + c + 1, :] = shared_index[c]

    dead_rows = jnp.zeros((pad - trace, width), F32)
    for k in range(blocks):
        for i in (1, 3):
            h_recv[i, k, trace:pad, :] = dead_rows
        for c in range(blocks):
            x_recv[k * blocks + c, trace:pad, :] = dead_rows

    @pl.when(cross < blocks * blocks)
    def _():
        empty = jnp.zeros((pad, width), F32)
        no_index = jnp.where(
            lax.broadcasted_iota(jnp.int32, (pad, width), 0) < trace, 0.0, -1.0
        )
        for k in range(blocks):
            owner = me - offsets[k]

            @pl.when(~valid(owner))
            def _():
                h_recv[0, k] = no_index

            for i in (1, 3):

                @pl.when(~valid(me - step_of(i, k)))
                def _():
                    h_recv[i, k] = empty

            for c in range(blocks):

                @pl.when(~(valid(owner) & valid(owner + offsets[c])))
                def _():
                    x_recv[k * blocks + c] = empty

    pl.semaphore_wait(barrier, count_valid(*(me + o for o in offsets)))
    start_all(0)

    for copy in in_copies[3:]:
        copy.wait()

    def face_index(t, s):
        return fm_ref[s : s + 1, t * LANES : (t + 1) * LANES]

    def pick_own(rnd):
        for t in range(tiles):
            for s in range(sides):
                picked[t, s] = pick_tile(
                    own_tile(rnd), 0, own_tiles, face_index(t, s), jnp.zeros((pad, LANES), F32)
                )

    pick_own(0)

    lo_iota = lax.broadcasted_iota(jnp.int32, (WIDE, LANES), 0)

    def one_hot(test):
        return jnp.where(test, 1.0, 0.0).astype(BF16)

    for t in range(tiles):
        for s in range(sides):
            lane = (t * sides + s) * LANES
            low = face_index(t, s) & (WIDE - 1)
            pick_map[:, lane : lane + LANES] = one_hot(lo_iota == low)
    for k in range(blocks):
        low = jnp.where(alive[k], send_index[k] & (WIDE - 1), -1)
        send_map[:, k * width : (k + 1) * width] = one_hot(lo_iota == low)
    prod[...] = jnp.zeros_like(prod)
    diag_row = mass_ref[...] + absorb_ref[...].astype(F32) * imp_ref[...]

    def column_of(row):
        dead_apart = jnp.where(row < 0.0, -2.0, row)
        return jnp.transpose(jnp.broadcast_to(dead_apart, (width, width)))

    def map_shared():
        for k in range(blocks):
            rows = [h_recv[0, k, trace + c : trace + c + 1, :] for c in range(blocks)]
            for c in range(blocks):
                same_map[k, c * width : (c + 1) * width, :] = one_hot(column_of(rows[c]) == rows[k])

    def map_returned():
        for k in range(blocks):
            column = column_of(shared_index[k])
            for t in range(tiles):
                for s in range(sides):
                    lane = (t * sides + s) * LANES
                    pick_same[k * width : (k + 1) * width, lane : lane + LANES] = one_hot(
                        column == face_index(t, s).astype(F32)
                    )

    pairs = dofs // 2
    body = dofs - 8

    def product(t):
        def row_at(ref, j):
            at = j // trace * pad + j % trace
            return jnp.broadcast_to(ref[t, at : at + 1, :], (8, LANES))

        def run(first, blocks, inputs):
            total = [None] * blocks
            for jj in range(pairs):
                at = jj * 2 * dofs + first
                high, low = (inputs(ref, jj).astype(BF16) for ref in (x_high, x_low))
                for i in range(blocks):
                    matrix = em_buf[t, at + i * 16 : at + i * 16 + 16, :]
                    for x in (high, low):
                        term = matrix.astype(F32) * x.astype(F32)
                        total[i] = term if jj == 0 and x is high else total[i] + term
            return total

        def rows(first, second):
            return lambda ref, jj: jnp.concatenate(
                [row_at(ref, 2 * jj + first), row_at(ref, 2 * jj + second)], axis=0
            )

        even = run(0, body // 16, rows(0, 0))
        odd = run(dofs + 8, body // 16, rows(1, 1))
        mixed = run(body, 1, rows(0, 1))[0]
        return jnp.concatenate(even + [mixed[:8]], axis=0) + jnp.concatenate(
            [mixed[8:]] + odd, axis=0
        )

    def side_values(t, s):
        value = prod[t, s * trace : s * trace + pad, :]
        return jnp.concatenate(
            [value[: pad - 8], jnp.where(row_live, value[pad - 8 :], 0.0)], axis=0
        )

    def spread(t, first_hi, count):
        parts = []
        for s in range(sides):
            value = side_values(t, s)
            high = jnp.broadcast_to(face_index(t, s) >> 8, (pad, LANES))
            parts.append(
                split2(
                    jnp.concatenate(
                        [jnp.where(high == first_hi + h, value, 0.0) for h in range(count)], axis=0
                    )
                )
            )
        lane = t * sides * LANES
        return dot_nt(
            jnp.concatenate(parts, axis=1), pick_map[:, lane : lane + sides * LANES]
        )

    def elements_of(rnd):
        ghost_total = None
        for t in range(tiles):
            for s in range(sides):
                value = pick_tile(
                    lambda h: h_recv[2 * rnd, h],
                    own_tiles, ghost_tiles, face_index(t, s), picked[t, s],
                )
                picked[t, s] = value
                high = value.astype(BF16).astype(F32)
                x_high[t, s * pad : (s + 1) * pad, :] = high
                x_low[t, s * pad : (s + 1) * pad, :] = value - high
            prod[t, 0:dofs, :] = product(t)
        for t in range(tiles):
            part = spread(t, own_hi, ghost_hi)
            ghost_total = part if ghost_total is None else ghost_total + part
        ghost_total = sum2(ghost_total)
        per_wide = WIDE // width
        for k in range(blocks):
            h, lane = k // per_wide, k % per_wide * width
            h_send[2 * rnd + 1, k] = ghost_total[h * pad : (h + 1) * pad, lane : lane + width]

    def energy_of():
        energy = None
        for t in range(tiles):
            for s in range(sides):
                term = picked[t, s] * side_values(t, s)
                energy = term if energy is None else energy + term
        return lane_sums(energy)

    def own_sums(rnd):
        total = None
        for t in range(tiles):
            part = spread(t, 0, own_hi)
            total = part if total is None else total + part
        total = sum2(total)
        for h in range(own_hi):
            lanes = slice(h * WIDE, (h + 1) * WIDE)
            own_buf[rnd + 1, :, lanes] = (
                total[h * pad : (h + 1) * pad] + own_buf[rnd, :, lanes] * diag_row[:, lanes]
            )

    def add_returned(rnd):
        parts = []
        for k in range(blocks):
            value = h_recv[2 * rnd + 1, k]
            high = jnp.broadcast_to(send_index[k] >> 8, (pad, LANES))
            parts.append(
                split2(
                    jnp.concatenate(
                        [jnp.where(high == i, value, 0.0) for i in range(own_hi)], axis=0
                    )
                )
            )
        total = sum2(dot_nt(jnp.concatenate(parts, axis=1), send_map[...]))
        for h in range(own_hi):
            lanes = slice(h * WIDE, (h + 1) * WIDE)
            own_buf[rnd + 1, :, lanes] += total[h * pad : (h + 1) * pad]

    def lane_sums(x):
        total = jnp.sum(x, axis=0, keepdims=True)
        while total.shape[1] > LANES:
            half = total.shape[1] // 2
            total = total[:, :half] + total[:, half:]
        return total

    lane_of = lax.broadcasted_iota(jnp.int32, (1, LANES), 1)
    quarter = LANES // 4
    lane_parts = (
        lane_of < quarter,
        (lane_of >= quarter) & (lane_of < 2 * quarter),
        lane_of >= 2 * quarter,
    )

    def fold(x, lanes):
        x = jnp.broadcast_to(x, (8, LANES))
        size = LANES // 2
        while size >= lanes:
            x = x + pltpu.roll(x, size, 1)
            size //= 2
        return x[0:1]

    def one_row(x, y, z):
        rest = jnp.where(lane_parts[1], fold(y, quarter), fold(z, 2 * quarter))
        return jnp.where(lane_parts[0], fold(x, quarter), rest)

    def begin_sum(rows):
        sums[me] = jnp.concatenate(rows, axis=0)
        for d in range(n - 1):
            pltpu.make_async_remote_copy(
                src_ref=sums.at[me], dst_ref=sums.at[me],
                send_sem=s_send_sem, recv_sem=s_recv_sem,
                device_id=(d + (d >= me).astype(jnp.int32),), device_id_type=MESH,
            ).start()

    def sum_wait(sem):
        ref = sums.at[pl.ds(0, n - 1)]
        pltpu.make_async_copy(ref, ref, sem).wait()

    def end_sum():
        sum_wait(s_recv_sem)
        total = jnp.sum(sums[...], axis=0)
        first = total[0:1]
        rows = [jnp.where(part, first, 0.0) for part in lane_parts] + [total[1:2]]
        total = jnp.sum(jnp.concatenate(rows, axis=0), axis=1, keepdims=True)
        return [total[i : i + 1] for i in range(4)]

    pltpu.make_async_copy(em_buf, em_buf, em_sem).wait()
    wait_recv(0)
    if reaches:
        spread_word(0)
    elements_of(0)
    start_all(1)
    for copy, to in relays():
        pl.when(to)(copy.start)
    own_sums(0)
    for k in range(blocks):
        h_send[2, k] = send_values(1, k)
    for copy, to in owners():
        pl.when(to)(copy.start)
    pass_word(0)
    b = own_buf[0]
    b_square = lane_sums(b * b)
    b_energy = energy_of() + lane_sums(b * b * diag_row)
    map_shared()
    map_returned()
    pick_own(1)
    pass_word(1)

    wait_recv(1)
    returned = split2(jnp.concatenate([h_recv[1, k] for k in range(blocks)], axis=1))
    for t in range(tiles):
        lane = t * sides * LANES
        extra = sum2(dot(returned, pick_same[:, lane : lane + sides * LANES]))
        for s in range(sides):
            picked[t, s] += extra[:, s * LANES : (s + 1) * LANES]
    add_returned(0)
    q = own_buf[1]
    q_square = lane_sums(q * q)
    q_diagonal = lane_sums(q * q * diag_row)
    early_row = one_row(b_square, b_energy, q_square)
    wait_count(cross, cross_choices, cross_view, h_recv_sem.at[2])
    for k in range(blocks):
        parts = jnp.concatenate(
            [h_send[1, k] if c == k else x_recv[k * blocks + c] for c in range(blocks)], axis=1
        )
        h_recv[2, k] = x_recv[k * blocks + k] + sum2(dot(split2(parts), same_map[k]))

    elements_of(1)
    for i in range(2, len(reaches)):
        pass_word(i)
    begin_sum([early_row, energy_of() + q_diagonal])
    start_all(3)
    own_sums(1)
    wait_recv(3)
    add_returned(1)
    rr, curve, q_norm, q_energy = end_sum()
    step0 = rr / curve
    new = step0 * step0 * q_norm - rr
    beta = new * (1.0 / rr)
    r1_energy = curve - 2.0 * step0 * q_norm + step0 * step0 * q_energy
    step1 = new / (r1_energy - beta * beta * curve)
    b, q, w = own_buf[0, 0:trace], own_buf[1, 0:trace], own_buf[2, 0:trace]
    r1 = b - step0 * q
    sol_ref[...] = step0 * b + step1 * (r1 + beta * b)
    res_ref[...] = r1 - step1 * (q - step0 * w + beta * q)
    wait_count(near, near_choices, lambda count: h_send.at[0, pl.ds(0, count)], h_send_sem.at[0])
    wait_count(
        near,
        near_choices,
        lambda count: h_send.at[pl.ds(1, 2), pl.ds(0, count), pl.ds(0, trace)],
        h_send_sem.at[1],
    )
    wait_count(cross, cross_choices, cross_view, h_send_sem.at[2])
    sum_wait(s_send_sem)


def put_out(sol_ref, res_ref, sol_out, res_out, sems):
    copies = [
        pltpu.make_async_copy(sol_ref, sol_out, sems.at[0]),
        pltpu.make_async_copy(res_ref, res_out, sems.at[1]),
    ]
    for copy in copies:
        copy.start()
    for copy in copies:
        copy.wait()


def solution(mesh):
    n = mesh.shape["dom"]

    def shards(rs, em, fm, si, sc, mass, absorb, imp):
        trace, own = rs.shape
        sides, elements = fm.shape
        blocks, width = si.shape[1:]
        pad = -(-trace // 8) * 8
        dofs = sides * trace
        tiles = elements // LANES
        ghost = blocks * width
        words = sum(2 * (blocks // 2) << i < n - 1 for i in range(n)) or 1
        assert width == LANES and dofs % 16 == 8 and trace + blocks <= pad
        cfg = (n, trace, sides, elements, own, blocks, width)
        dma = pltpu.SemaphoreType.DMA
        vmem = pl.BlockSpec(memory_space=pltpu.VMEM)
        sol, res = pl.pallas_call(
            functools.partial(kernel, cfg),
            out_shape=[pltpu.VMEM(rs.shape, F32)] * 2,
            in_specs=[pl.BlockSpec(memory_space=pltpu.HBM)] * 8,
            out_specs=[vmem] * 2,
            scratch_shapes=[
                pltpu.VMEM(rs.shape, F32),
                pltpu.VMEM(fm.shape, jnp.int32),
                pltpu.VMEM(si.shape, jnp.int32),
                pltpu.VMEM(sc.shape, jnp.int32),
                pltpu.VMEM((1, own), F32),
                pltpu.VMEM((1, own), jnp.int32),
                pltpu.VMEM((1, own), F32),
                pltpu.VMEM((tiles, dofs * dofs, LANES), BF16),
                pltpu.VMEM((WIDE, sides * elements), BF16),
                pltpu.VMEM((WIDE, ghost), BF16),
                pltpu.VMEM((blocks, ghost, width), BF16),
                pltpu.VMEM((ghost, sides * elements), BF16),
                pltpu.VMEM((4, blocks, pad, width), F32),
                pltpu.VMEM((4, blocks, pad, width), F32),
                pltpu.VMEM((blocks * blocks, pad, width), F32),
                pltpu.VMEM((3, pad, own), F32),
                pltpu.VMEM((tiles, sides, pad, LANES), F32),
                pltpu.VMEM((tiles, sides * pad, LANES), F32),
                pltpu.VMEM((tiles, sides * pad, LANES), F32),
                pltpu.VMEM((tiles, dofs + 8, LANES), F32),
                pltpu.VMEM((n, 2, LANES), F32),
                dma((7,)), dma(()), dma((3,)), dma((4,)), dma(()), dma(()),
                pltpu.SemaphoreType.REGULAR((words,)),
            ],
            compiler_params=pltpu.CompilerParams(
                collective_id=0, has_side_effects=True, vmem_limit_bytes=62 * 1024 * 1024
            ),
        )(
            rs, em.reshape(dofs * dofs, elements), fm, si, sc,
            mass.reshape(1, own), absorb.reshape(1, own), imp.reshape(1, own),
        )
        return pl.pallas_call(
            put_out,
            out_shape=[jax.ShapeDtypeStruct(rs.shape, F32)] * 2,
            in_specs=[vmem] * 2,
            out_specs=[pl.BlockSpec(memory_space=pltpu.HBM)] * 2,
            scratch_shapes=[dma((2,))],
            compiler_params=pltpu.CompilerParams(vmem_limit_bytes=8 * 1024 * 1024),
        )(sol, res)

    placed = (
        P(None, "dom"),
        P(None, None, "dom"),
        P(None, "dom"),
        P("dom", None, None),
        P("dom", None),
        P("dom"),
        P("dom"),
        P("dom"),
    )
    return jax.shard_map(
        shards,
        mesh=mesh,
        in_specs=placed,
        out_specs=(P(None, "dom"), P(None, "dom")),
        check_vma=False,
    )
```
